32 devices in a mesh: dp: 8 (over y, x, core), mp: 4 (over z).
Axes of the slice: x: 2, y: 2, z: 4, core: 2. Of those that a mesh axis runs over, the one named last changes fastest.
Arguments:
- hidden: bfloat16 [12288, 1024], P(('dp', 'mp')), may hold values from -6 to 6
- lengths: int32 [8], P('dp'), may hold values from 1 to 1536, 7372 in all
- first_gain: float32 [1024], replicated, may hold values from 0.5 to 1.5
- first_shift: float32 [1024], replicated, may hold values from -1.75 to 1.75
- projection_in: bfloat16 [1024, 3, 1024], P(None, None, 'mp'), may hold values from -0.1875 to 0.1875
- query_value_bias: float32 [2, 1024], P(None, 'mp'), may hold values from -0.625 to 0.625
- projection_out: bfloat16 [1024, 1024], P('mp'), may hold values from -2 to 2
- out_bias: float32 [1024], replicated, may hold values from -1.75 to 1.75
- second_gain: float32 [1024], replicated, may hold values from 0.5 to 1.5
- second_shift: float32 [1024], replicated, may hold values from -1.75 to 1.75
- up_weight: bfloat16 [1024, 4096], P(None, 'mp'), may hold values from -0.1875 to 0.1875
- up_bias: bfloat16 [4096], P('mp'), may hold values from -1.75 to 1.75
- down_weight: bfloat16 [4096, 1024], P('mp'), may hold values from -0.09375 to 0.09375
- down_bias: float32 [1024], replicated, may hold values from -1.75 to 1.75
- cotangent: bfloat16 [12288, 1024], P(('dp', 'mp')), may hold values from -6 to 6
Outputs:
- output: bfloat16 [12288, 1024], P(('dp', 'mp'))
- gradient_hidden: bfloat16 [12288, 1024], P(('dp', 'mp'))
- gradient_first_gain: float32 [1024], replicated
- gradient_first_shift: float32 [1024], replicated
- gradient_projection_in: float32 [1024, 3, 1024], P('dp', None, 'mp')
- gradient_query_value_bias: float32 [2, 1024], replicated
- gradient_projection_out: float32 [1024, 1024], P('mp', 'dp')
- gradient_out_bias: float32 [1024], replicated
- gradient_second_gain: float32 [1024], replicated
- gradient_second_shift: float32 [1024], replicated
- gradient_up_weight: float32 [1024, 4096], P('dp', 'mp')
- gradient_up_bias: float32 [4096], replicated
- gradient_down_weight: float32 [4096, 1024], P('mp', 'dp')
- gradient_down_bias: float32 [1024], replicated
The draws below stay inside these ranges and needn't reach their ends.
Inputs may be any that keep to these rules, and one draw needn't show every extreme that they name: `lengths`: each utterance has at least one frame and at most 1536; the longest has exactly 1536.
All inputs are finite; a program needn't handle non-finite values. No bound on the sum of `lengths` on one device may be relied on, other than what follows from the above.
Results may differ from the reference program's by a relative error of at most 0.019.
Values may be sent and summed in bfloat16 or wider, within the bound.
No kernel may reach another device: no remote copies, remote signals or barrier semaphores. Data moves between devices by JAX's collectives and lax.ppermute only.
A program may use at most 128 MiB of HBM per device.

```python
import math
import jax
import jax.numpy as jnp
import numpy as np
from jax import lax

D = 1024
HEADS = 16
HEAD_DIM = 64
FF = 4096
LEN = 1536
BLOCK = 512
SEQS = 8
TOKENS = 12288


def shard_levels(own_key, dims, pieces, smallest, largest):
    factor_of, own = 1.0, jax.random.fold_in(own_key, 6)
    for dim, shards_of in pieces:
        heights = jnp.exp(jax.random.uniform(jax.random.fold_in(own, dim), (shards_of,), jnp.float32, smallest / len(pieces), largest / len(pieces)))
        factor_of = factor_of * jnp.repeat(heights, dims[dim] // shards_of).reshape([-1 if axis == dim else 1 for axis in range(len(dims))])
    return factor_of


def split_up(count, total, limit, skew):
    weights = [(1 << 20) // math.isqrt(standing ** skew) + 1 for standing in range(2, count + 1)]
    spare, holding = total - limit - (count - 1), [1] * (count - 1)
    while spare > 0:
        free = [i for i in range(count - 1) if holding[i] < limit]
        whole, remaining = sum([weights[i] for i in free]), spare
        for i in free:
            addition = min(limit - holding[i], max(1, remaining * weights[i] // whole), spare)
            holding[i] = holding[i] + addition
            spare = spare - addition
    return np.array([limit] + holding)


def ragged(stream_key, amount, total, bound, skew):
    if amount == 2:
        one = jax.random.randint(stream_key, (), max(1, total - bound), min(bound, total - 1) + 1)
        return jnp.stack([one, total - one])
    sizes = jnp.asarray(split_up(amount, total, bound, skew), jnp.int32)
    twos = (amount - 1) // 2
    giver, taker = sizes[1:1 + 2 * twos:2], sizes[2:2 + 2 * twos:2]
    margin = jnp.minimum(giver - 1, bound - taker)
    shifted = jax.random.randint(jax.random.fold_in(stream_key, 1), (twos,), 0, 1 << 20) % (margin + 1)
    sizes = sizes.at[1:1 + 2 * twos:2].set(giver - shifted).at[2:2 + 2 * twos:2].set(taker + shifted)
    return sizes[jax.random.permutation(jax.random.fold_in(stream_key, 2), amount)]


def scatter_about(stream_key, shape, width, limit, pieces=(), kind=jnp.bfloat16):
    drawn = jax.random.normal(stream_key, shape, jnp.float32) * width
    if len(pieces) > 0:
        drawn = shard_levels(stream_key, shape, pieces, -0.22, 0.18) * drawn
    return jnp.clip(drawn, min=-limit, max=limit).astype(kind)


def setup_inputs(seed: int = 0) -> dict:
    splits = jax.random.split(jax.random.key(seed), 16)
    return {
        "hidden": scatter_about(splits[0], (TOKENS, D), 1.0, 6.0, ((0, 32),)),
        "lengths": ragged(splits[1], SEQS, SEQS * LEN * 3 // 5, LEN, 1).astype(jnp.int32),
        "first_gain": jnp.clip(1.0 + 0.1 * jax.random.normal(splits[2], (D,), jnp.float32), 0.5, 1.5),
        "first_shift": scatter_about(splits[3], (D,), 0.3, 1.75, (), jnp.float32),
        "projection_in": scatter_about(splits[4], (D, 3, D), D ** -0.5, 0.1875, ((2, 4),)),
        "query_value_bias": scatter_about(splits[5], (2, D), 0.1, 0.625, ((1, 4),), jnp.float32),
        "projection_out": scatter_about(splits[6], (D, D), (max(D // 128, 4)) ** -0.5, 2.0, ((0, 4),)),
        "out_bias": scatter_about(splits[7], (D,), 0.3, 1.75, (), jnp.float32),
        "second_gain": jnp.clip(1.0 + 0.1 * jax.random.normal(splits[8], (D,), jnp.float32), 0.5, 1.5),
        "second_shift": scatter_about(splits[9], (D,), 0.3, 1.75, (), jnp.float32),
        "up_weight": scatter_about(splits[10], (D, FF), D ** -0.5, 0.1875, ((1, 4),)),
        "up_bias": scatter_about(splits[11], (FF,), 0.3, 1.75, ((0, 4),)),
        "down_weight": scatter_about(splits[12], (FF, D), FF ** -0.5, 0.09375, ((0, 4),)),
        "down_bias": scatter_about(splits[13], (D,), 0.3, 1.75, (), jnp.float32),
        "cotangent": scatter_about(splits[14], (TOKENS, D), 1.0, 6.0, ((0, 32),)),
    }


@jax.custom_vjp
def low(v):
    return lax.optimization_barrier(v.astype(jnp.bfloat16)).astype(jnp.float32)

@jax.custom_vjp
def low_back(v):
    return v

def low_keep(v):
    return (low(v), None)

def low_pass(kept, grad):
    return (grad,)

def back_keep(v):
    return (v, None)

def back_low(kept, grad):
    return (low(grad),)
low.defvjp(low_keep, low_pass)
low_back.defvjp(back_keep, back_low)
EPS = 1e-05
NEGATIVE = -1e+30

def layer_norm(values, gain, shift):
    centered = values - lax.optimization_barrier(jnp.mean(values, -1, keepdims=True))
    inverse = lax.rsqrt(lax.optimization_barrier(jnp.mean(centered * centered, -1, keepdims=True)) + EPS)
    return centered * inverse * gain + shift

def product(left, right):
    return jnp.dot(left, right, precision=lax.Precision.HIGHEST)

def layer(hidden, lengths, params):
    first_gain, first_shift, projection_in, query_value_bias, projection_out, out_bias, second_gain, second_shift, up_weight, up_bias, down_weight, down_bias = params
    scale = HEAD_DIM ** (-0.5)
    positions = jnp.arange(LEN, dtype=jnp.int32)
    starts = jnp.arange(LEN // BLOCK, dtype=jnp.int32) * BLOCK

    def utterance(pair):
        stream, length = pair
        first_normed = low(layer_norm(stream, first_gain, first_shift))
        projected = product(first_normed, projection_in.reshape(D, 3 * D)).reshape(LEN, 3, D)
        queries = low_back(low((projected[:, 0] + query_value_bias[0]) * scale)).reshape(LEN, HEADS, HEAD_DIM)
        keys_all = low_back(low(projected[:, 1])).reshape(LEN, HEADS, HEAD_DIM)
        values_all = low_back(low(projected[:, 2] + query_value_bias[1])).reshape(LEN, HEADS, HEAD_DIM)

        def block(start):
            query_block = lax.dynamic_slice_in_dim(queries, start, BLOCK, 0)
            scores = low_back(jnp.einsum('qhd,khd->hqk', query_block, keys_all, precision=lax.Precision.HIGHEST))
            row_at = start + jnp.arange(BLOCK, dtype=jnp.int32)
            allowed = (positions[None, :] <= row_at[:, None]) & (positions[None, :] < length)
            scores = jnp.where(allowed[None], scores, NEGATIVE)
            weights = low(jnp.exp(scores - jax.nn.logsumexp(scores, axis=-1, keepdims=True)))
            context = jnp.einsum('hqk,khd->qhd', weights, values_all, precision=lax.Precision.HIGHEST)
            return low_back(low(context)).reshape(BLOCK, D)
        context = lax.map(jax.checkpoint(block), starts).reshape(LEN, D)
        middle = stream + low_back(product(context, projection_out)) + out_bias
        second_normed = low(layer_norm(middle, second_gain, second_shift))
        before = low_back(product(second_normed, up_weight) + up_bias)
        activated = low(jax.nn.gelu(before, approximate=False))
        return middle + low_back(product(activated, down_weight)) + down_bias
    result = lax.map(jax.checkpoint(utterance), (hidden.reshape(SEQS, LEN, D), lengths))
    return result.reshape(TOKENS, D)

def reference(hidden, lengths, first_gain, first_shift, projection_in, query_value_bias, projection_out, out_bias, second_gain, second_shift, up_weight, up_bias, down_weight, down_bias, cotangent):
    params = tuple((item.astype(jnp.float32) for item in (first_gain, first_shift, projection_in, query_value_bias, projection_out, out_bias, second_gain, second_shift, up_weight, up_bias, down_weight, down_bias)))
    stream = hidden.astype(jnp.float32)
    result, pullback = jax.vjp(lambda values, weights: layer(values, lengths, weights), stream, params)
    back_stream, grads = pullback(cotangent.astype(jnp.float32))
    return (result.astype(jnp.bfloat16), back_stream.astype(jnp.bfloat16), grads[0], grads[1], grads[2], grads[3], grads[4], grads[5], grads[6], grads[7], grads[8], grads[9], grads[10], grads[11])
```

```python
import jax
import jax.numpy as jnp
from jax import lax
from jax.experimental import pallas as pl
from jax.experimental.pallas import tpu as pltpu
from jax.sharding import PartitionSpec as P

HEAD_DIM = 64
TILE = 256
NEGATIVE = -1e30

def mm(left, right):
    return jnp.dot(left, right, preferred_element_type=jnp.float32)

def split_three(value):
    high = value.astype(jnp.bfloat16)
    rest = value - high.astype(jnp.float32)
    low = rest.astype(jnp.bfloat16)
    return high, low, (rest - low.astype(jnp.float32)).astype(jnp.bfloat16)

def forward_kernel(length_ref, q_ref, k_ref, v_ref, context_ref, total_ref, q_turned, v_turned, keys_at, out_turned):
    rows, width = q_ref.shape
    heads = width // HEAD_DIM
    length = length_ref[0]
    q_turned[...] = q_ref[...].T
    v_turned[...] = v_ref[...].T
    key_row = lax.broadcasted_iota(jnp.int32, (rows, width), 0)
    lane = lax.broadcasted_iota(jnp.int32, (rows, width), 1)
    feature = lax.broadcasted_iota(jnp.int32, (width, TILE), 0)
    key_at = lax.broadcasted_iota(jnp.int32, (TILE, TILE), 0)
    query_at = lax.broadcasted_iota(jnp.int32, (TILE, TILE), 1)

    def one_head(head, _):
        first = pl.multiple_of(head * HEAD_DIM, HEAD_DIM)
        spare = lax.rem(head + 1, heads) * HEAD_DIM
        off = jnp.where(key_row < length, 0.0, NEGATIVE).astype(jnp.bfloat16)
        keys_at[...] = jnp.where(lane == spare, off, k_ref[...])
        for tile in range(rows // TILE):
            cols = slice(tile * TILE, (tile + 1) * TILE)
            count = (tile + 1) * TILE
            query = q_turned[:, cols]
            query = jnp.where(feature // HEAD_DIM == head, query, jnp.where(feature == spare, 1.0, 0.0).astype(jnp.bfloat16))
            scores = mm(keys_at[:count, :], query)
            last = jnp.where(key_at <= query_at, scores[tile * TILE :], NEGATIVE)
            highest = jnp.max(last, 0, keepdims=True)
            if tile:
                highest = jnp.maximum(highest, jnp.max(scores[: tile * TILE], 0, keepdims=True))
            weights = jnp.exp(last - highest)
            total = jnp.sum(weights, 0, keepdims=True)
            low = weights.astype(jnp.bfloat16)
            if tile:
                before = jnp.exp(scores[: tile * TILE] - highest)
                total = total + jnp.sum(before, 0, keepdims=True)
                low = jnp.concatenate([before.astype(jnp.bfloat16), low], 0)
            out = mm(v_turned[pl.ds(first, HEAD_DIM), :count], low)
            out_turned[pl.ds(first, HEAD_DIM), cols] = out / total
            total_ref[pl.ds(head, 1), cols] = highest + jnp.log(total)
        return 0

    lax.fori_loop(0, heads, one_head, 0)
    context_ref[...] = out_turned[...].T.astype(jnp.bfloat16)

def attend(queries, keys, values, length):
    rows, width = queries.shape
    whole = lambda: pl.BlockSpec(memory_space=pltpu.VMEM)
    return pl.pallas_call(
        forward_kernel,
        out_shape=(jax.ShapeDtypeStruct((rows, width), jnp.bfloat16), jax.ShapeDtypeStruct((8, rows), jnp.float32)),
        in_specs=[pl.BlockSpec(memory_space=pltpu.SMEM), whole(), whole(), whole()],
        out_specs=(whole(), whole()),
        scratch_shapes=[
            pltpu.VMEM((width, rows), jnp.bfloat16),
            pltpu.VMEM((width, rows), jnp.bfloat16),
            pltpu.VMEM((rows, width), jnp.bfloat16),
            pltpu.VMEM((width, rows), jnp.float32),
        ],
        compiler_params=pltpu.CompilerParams(vmem_limit_bytes=48 << 20),
        cost_estimate=pl.CostEstimate(flops=2 * rows * rows * width * 2, bytes_accessed=8 * rows * width, transcendentals=rows * rows * 2),
        name="attend",
    )(length, queries, keys, values)

def backward_kernel(length_ref, q_ref, k_ref, v_ref, c_ref, g_ref, total_ref, dq_ref, dk_ref, dv_ref,
                    q_turned, k_turned, g_turned, product, q_side, g_side, q_head, g_head, dq_turned, dk_sum, dv_sum):
    rows, width = q_ref.shape
    heads = width // HEAD_DIM
    length = length_ref[0]
    q_turned[...] = q_ref[...].T
    k_turned[...] = k_ref[...].T
    g_turned[...] = g_ref[...].T
    product[...] = (g_ref[...].astype(jnp.float32) * c_ref[...].astype(jnp.float32)).T
    dk_sum[...] = jnp.zeros_like(dk_sum)
    dv_sum[...] = jnp.zeros_like(dv_sum)
    lane_all = lax.broadcasted_iota(jnp.int32, (rows, width), 1)
    feature = lax.broadcasted_iota(jnp.int32, (width, rows), 0)
    lane = lax.broadcasted_iota(jnp.int32, (TILE, width), 1)
    key_at = lax.broadcasted_iota(jnp.int32, (TILE, TILE), 0)
    query_at = lax.broadcasted_iota(jnp.int32, (TILE, TILE), 1)
    none = jnp.zeros((), jnp.bfloat16)

    def one_head(head, _):
        first = pl.multiple_of(head * HEAD_DIM, HEAD_DIM)
        spare = lax.rem(head + 1, heads) * HEAD_DIM
        total = total_ref[pl.ds(head, 1), :]
        inner = jnp.sum(product[pl.ds(first, HEAD_DIM), :], 0, keepdims=True)
        mine = feature // HEAD_DIM == head
        def side(turned, taken, one):
            high, low, least = split_three(-taken)
            extra = jnp.where(feature == spare, high, jnp.where(feature == spare + 1, low, jnp.where(feature == spare + 2, least,
                jnp.where(feature == spare + 3, one, none))))
            return jnp.where(mine, turned, extra)
        q_side[...] = side(q_turned[...], total, jnp.ones((), jnp.bfloat16))
        g_side[...] = side(g_turned[...], inner, none)
        own = lane_all // HEAD_DIM == head
        q_head[...] = jnp.where(own, q_ref[...], none)
        g_head[...] = jnp.where(own, g_ref[...], none)
        for tile in range(rows // TILE):
            at = slice(tile * TILE, (tile + 1) * TILE)
            key_row = lax.broadcasted_iota(jnp.int32, (TILE, width), 0) + tile * TILE
            off = jnp.where(key_row < length, 0.0, NEGATIVE).astype(jnp.bfloat16)
            ones = (lane >= spare) & (lane < spare + 3)
            one = jnp.ones((), jnp.bfloat16)
            keys = jnp.where(ones, one, jnp.where(lane == spare + 3, off, k_ref[at, :]))
            values = jnp.where(ones, one, v_ref[at, :])
            scores = mm(keys, q_side[:, tile * TILE :])
            back = mm(values, g_side[:, tile * TILE :])
            weights = jnp.exp(scores)
            near = jnp.where(key_at <= query_at, weights[:, :TILE], 0.0)
            if tile + 1 < rows // TILE:
                weights = jnp.concatenate([near, weights[:, TILE:]], 1)
            else:
                weights = near
            low = weights.astype(jnp.bfloat16)
            back_scores = (weights * back).astype(jnp.bfloat16)
            dv_sum[at, :] += mm(low, g_head[tile * TILE :, :])
            dk_sum[at, :] += mm(back_scores, q_head[tile * TILE :, :])
            dq = mm(k_turned[pl.ds(first, HEAD_DIM), at], back_scores)
            if tile:
                dq_turned[pl.ds(first, HEAD_DIM), tile * TILE :] += dq
            else:
                dq_turned[pl.ds(first, HEAD_DIM), :] = dq
        return 0

    lax.fori_loop(0, heads, one_head, 0)
    dq_ref[...] = (dq_turned[...].T.astype(jnp.bfloat16).astype(jnp.float32) * HEAD_DIM**-0.5).astype(jnp.bfloat16)
    dk_ref[...] = dk_sum[...].astype(jnp.bfloat16)
    dv_ref[...] = dv_sum[...].astype(jnp.bfloat16)

def attend_back(queries, keys, values, context, back_context, total, length):
    rows, width = queries.shape
    whole = lambda: pl.BlockSpec(memory_space=pltpu.VMEM)
    flat = jax.ShapeDtypeStruct((rows, width), jnp.bfloat16)
    low, wide = jnp.bfloat16, jnp.float32
    return pl.pallas_call(
        backward_kernel,
        out_shape=(flat, flat, flat),
        in_specs=[pl.BlockSpec(memory_space=pltpu.SMEM)] + [whole()] * 6,
        out_specs=(whole(), whole(), whole()),
        scratch_shapes=[
            pltpu.VMEM((width, rows), low), pltpu.VMEM((width, rows), low), pltpu.VMEM((width, rows), low),
            pltpu.VMEM((width, rows), wide), pltpu.VMEM((width, rows), low), pltpu.VMEM((width, rows), low),
            pltpu.VMEM((rows, width), low), pltpu.VMEM((rows, width), low), pltpu.VMEM((width, rows), wide),
            pltpu.VMEM((rows, width), wide), pltpu.VMEM((rows, width), wide),
        ],
        compiler_params=pltpu.CompilerParams(vmem_limit_bytes=56 << 20),
        cost_estimate=pl.CostEstimate(flops=5 * rows * rows * width * 2, bytes_accessed=20 * rows * width, transcendentals=rows * rows * 2),
        name="attend_back",
    )(length, queries, keys, values, context, back_context, total)

EPS = 1e-05


def normalize(values):
    centered = values - jnp.mean(values, -1, keepdims=True)
    inverse = lax.rsqrt(jnp.mean(centered * centered, -1, keepdims=True) + EPS)
    return (centered * inverse, inverse)


def norm_back(incoming, scaled_in, inverse, gain):
    weighted = incoming * gain
    return inverse * (
        weighted
        - jnp.mean(weighted, -1, keepdims=True)
        - scaled_in * jnp.mean(weighted * scaled_in, -1, keepdims=True)
    )


def over_rows(left, right):
    return lax.dot_general(left, right, (((0,), (0,)), ((), ())), preferred_element_type=jnp.float32)


def over_cols(left, right):
    return lax.dot_general(left, right, (((1,), (1,)), ((), ())), preferred_element_type=jnp.float32)


def feed_kernel(core_ref, x_ref, g_ref, up_ref, bias_ref, down_ref, act_ref, back_ref, sums_ref,
                out_own, out_other, x_own, x_other, out_sum, x_sum):
    step = pl.program_id(0)
    rows = x_ref.shape[0]
    half = rows // 2
    up, down = up_ref[0], down_ref[0]
    before = mm(x_ref[...], up) + bias_ref[0]
    inside = 0.5 * (1.0 + lax.erf(before * 0.5**0.5))
    slope = inside + before * (jnp.exp(-0.5 * before * before) * (0.5 / jnp.pi) ** 0.5)
    act = (before * inside).astype(jnp.bfloat16)
    back = (over_cols(g_ref[...], down) * slope).astype(jnp.bfloat16)
    act_ref[...] = act
    back_ref[...] = back
    sums_ref[0] = jnp.sum(back.astype(jnp.float32), 0, keepdims=True)
    out = mm(act, down)
    grad = over_cols(back, up)

    @pl.when(step == 0)
    def _():
        out_sum[...] = out
        x_sum[...] = grad

    @pl.when(step > 0)
    def _():
        out_sum[...] += out
        x_sum[...] += grad

    @pl.when(step == pl.num_programs(0) - 1)
    def _():
        out_own[...] = out_sum[:half, :]
        out_other[...] = out_sum[half:, :].astype(jnp.bfloat16)
        x_own[...] = x_sum[:half, :]
        x_other[...] = x_sum[half:, :].astype(jnp.bfloat16)


def feed(core, x, g, up, bias, down):
    rows, width = x.shape
    shards, _, hidden = up.shape
    part = hidden // 2
    low, wide = jnp.bfloat16, jnp.float32
    once = lambda shape: pl.BlockSpec(shape, lambda t, c: (0, 0))
    flat = lambda kind: jax.ShapeDtypeStruct((rows // 2, width), kind)
    return pl.pallas_call(
        feed_kernel,
        grid_spec=pltpu.PrefetchScalarGridSpec(
            num_scalar_prefetch=1,
            grid=(shards,),
            in_specs=[
                once((rows, width)),
                once((rows, width)),
                pl.BlockSpec((1, width, part), lambda t, c: (t, 0, c[0])),
                pl.BlockSpec((1, 1, part), lambda t, c: (t, 0, c[0])),
                pl.BlockSpec((1, part, width), lambda t, c: (t, c[0], 0)),
            ],
            out_specs=[
                pl.BlockSpec((rows, part), lambda t, c: (0, t)),
                pl.BlockSpec((rows, part), lambda t, c: (0, t)),
                pl.BlockSpec((1, 1, part), lambda t, c: (t, 0, 0)),
            ]
            + [once((rows // 2, width))] * 4,
            scratch_shapes=[pltpu.VMEM((rows, width), wide)] * 2,
        ),
        out_shape=(
            jax.ShapeDtypeStruct((rows, shards * part), low),
            jax.ShapeDtypeStruct((rows, shards * part), low),
            jax.ShapeDtypeStruct((shards, 1, part), wide),
            flat(wide),
            flat(low),
            flat(wide),
            flat(low),
        ),
        compiler_params=pltpu.CompilerParams(vmem_limit_bytes=56 << 20),
        cost_estimate=pl.CostEstimate(flops=8 * rows * width * shards * part, bytes_accessed=4 * shards * width * part, transcendentals=2 * rows * shards * part),
        name="feed",
    )(core, x, g, up, bias, down)


def turn(size, by):
    return [(at, (at + by) % size) for at in range(size)]


def flip(size, bit):
    return [(at, at ^ bit) for at in range(size)]


def add_up(values):
    for axis in ("dp", "mp"):
        bit = 1
        while bit < lax.axis_size(axis):
            values = values + lax.ppermute(values, axis, flip(lax.axis_size(axis), bit))
            bit *= 2
    return values


def body(hidden, lengths, first_gain, first_shift, projection_in, query_value_bias, projection_out, out_bias,
         second_gain, second_shift, up_weight, up_bias, down_weight, down_bias, cotangent):
    rows, width = hidden.shape
    heads_width = projection_in.shape[2]
    hidden_width = up_weight.shape[1]
    groups, members = lax.axis_size("dp"), lax.axis_size("mp")
    group, member = lax.axis_index("dp"), lax.axis_index("mp")
    core = group % 2
    half = hidden_width // 2
    scale = HEAD_DIM ** (-0.5)
    low, wide = jnp.bfloat16, jnp.float32
    both = ("mp", "dp")
    same_core = [list(range(at, groups, 2)) for at in range(2)]
    swap = lambda value: lax.ppermute(value, "dp", flip(groups, 1))
    pass_on = lambda value, by: lax.ppermute(value, "mp", turn(members, by))

    def gathered(weight):
        count = weight.shape[0] // groups
        piece = lax.dynamic_slice_in_dim(weight, group * count, count, 0)
        return lax.all_gather(piece, both, axis=0, tiled=True)

    stream = hidden.astype(wide)
    first_hat, first_inverse = normalize(stream)
    first_own = (first_hat * first_gain + first_shift).astype(low)
    bias_all = lax.all_gather(up_bias, "mp", axis=0, tiled=True).astype(wide).reshape(members, 1, hidden_width)
    out_full = gathered(projection_out)
    up_full = gathered(up_weight).reshape(members, width, hidden_width)
    down_full = gathered(down_weight).reshape(members, hidden_width, width)

    first_full = jnp.zeros((members * rows, width), low)
    held = first_own
    for by in range(members):
        first_full = lax.dynamic_update_slice_in_dim(first_full, held, (member - by) % members * rows, 0)
        if by < members - 1:
            held = pass_on(held, 1)
    weight_flat = projection_in.reshape(width, 3 * heads_width)
    projected = lambda at: jnp.dot(first_full, projection_in[:, at], preferred_element_type=wide)
    queries = ((projected(0) + query_value_bias[0]) * scale).astype(low)
    keys = projected(1).astype(low)
    values = (projected(2) + query_value_bias[1]).astype(low)
    context, total = attend(queries, keys, values, lengths)

    context_rows = jnp.zeros((rows, width), low)
    for by in range(members):
        part = lax.dynamic_slice_in_dim(context, (member + by) % members * rows, rows, 0)
        part = pass_on(part, by) if by else part
        context_rows = lax.dynamic_update_slice_in_dim(context_rows, part, (member - by) % members * heads_width, 1)
    middle = stream + jnp.dot(context_rows, out_full, preferred_element_type=wide) + out_bias
    second_hat, second_inverse = normalize(middle)
    second_own = (second_hat * second_gain + second_shift).astype(low)
    second_pair = jnp.concatenate([second_own, swap(second_own)], 0)
    cotangent_pair = jnp.concatenate([cotangent, swap(cotangent)], 0)
    activated, back_before, up_bias_part, out_own, out_other, back_own, back_other = feed(
        core.reshape(1), second_pair, cotangent_pair, up_full, bias_all, down_full
    )
    back_second = back_own + swap(back_other).astype(wide)
    output = (middle + out_own + swap(out_other).astype(wide) + down_bias).astype(low)
    out_grad = cotangent.astype(wide)
    second_gain_grad = jnp.sum(back_second * second_hat, 0)
    second_shift_grad = jnp.sum(back_second, 0)
    back_middle = out_grad + norm_back(back_second, second_hat, second_inverse, second_gain)
    low_middle = back_middle.astype(low)
    back_rows = over_cols(low_middle, out_full).astype(low)
    back_context = jnp.zeros((members * rows, heads_width), low)
    for by in range(members):
        part = lax.dynamic_slice_in_dim(back_rows, (member + by) % members * heads_width, heads_width, 1)
        part = pass_on(part, by) if by else part
        back_context = lax.dynamic_update_slice_in_dim(back_context, part, (member - by) % members * rows, 0)

    up_part = over_rows(second_pair, back_before).astype(low)
    down_part = over_rows(cotangent_pair, activated).astype(low)
    out_part = over_rows(low_middle, context_rows).astype(low)
    spread = lambda value: lax.psum_scatter(value, "dp", scatter_dimension=0, axis_index_groups=same_core, tiled=True)
    up_part, down_part, out_part = spread(up_part), spread(down_part), spread(out_part)

    def summed(chunk):
        held = chunk((member - 1) % members).astype(low)
        for by in range(2, members + 1):
            held = pass_on(held, 1).astype(wide) + chunk((member - by) % members)
            held = held.astype(low) if by < members else held
        return held

    def weight_chunk(at):
        return jnp.concatenate(
            [lax.dynamic_slice_in_dim(part, at * wide_of, wide_of, 1) for part, wide_of in ((up_part, half), (down_part, half), (out_part, heads_width))], 1
        ).astype(wide)

    weight_sum = summed(weight_chunk)
    count = width // groups
    kept = lax.dynamic_slice_in_dim(weight_sum, core * count, count, 0)
    given = lax.dynamic_slice_in_dim(weight_sum, (1 - core) * count, count, 0).astype(low)
    taken = swap(given).astype(wide)
    first_kept = core == 0
    ordered = lambda at: jnp.concatenate(
        [jnp.where(first_kept, kept[:, at], taken[:, at]), jnp.where(first_kept, taken[:, at], kept[:, at])], 1
    )
    up_grad = ordered(slice(0, half))
    down_grad = ordered(slice(half, 2 * half)).T
    out_weight_grad = (kept[:, 2 * half :] + taken[:, 2 * half :]).T

    back_queries, back_keys, back_values = attend_back(queries, keys, values, context, back_context, total, lengths)
    back_projected = jnp.concatenate([back_queries, back_keys, back_values], 1)
    projection_part = over_rows(first_full, back_projected)
    projection_grad = lax.psum_scatter(projection_part.astype(low), "dp", scatter_dimension=0, tiled=True)
    projection_grad = projection_grad.astype(wide).reshape(-1, 3, heads_width)
    weight_wide = weight_flat.astype(wide)
    projected_sums = jnp.sum(back_projected, 0, dtype=wide)
    first_shift_grad = jnp.sum(weight_wide * projected_sums, 1)
    first_gain_grad = (jnp.sum(weight_wide * projection_part, 1) - first_shift * first_shift_grad) / first_gain
    back_first = summed(
        lambda at: over_cols(lax.dynamic_slice_in_dim(back_projected, at * rows, rows, 0), weight_flat)
    )
    hidden_grad = (back_middle + norm_back(back_first, first_hat, first_inverse, first_gain)).astype(low)

    placed = lambda value, size, at: lax.dynamic_update_slice(jnp.zeros((size,), wide), value, (at,))
    up_bias_sums = jnp.zeros((members, 2, half), wide)
    up_bias_sums = lax.dynamic_update_slice(up_bias_sums, up_bias_part, (0, core, 0)).reshape(-1)
    sums = [
        first_gain_grad,
        first_shift_grad,
        placed(projected_sums[:heads_width], width, member * heads_width),
        placed(projected_sums[2 * heads_width :], width, member * heads_width),
        jnp.sum(back_middle, 0),
        second_gain_grad,
        second_shift_grad,
        jnp.sum(out_grad, 0),
        up_bias_sums,
    ]
    sums = add_up(jnp.concatenate(sums).reshape(-1, 128)).reshape(-1)
    small = [sums[at * width : (at + 1) * width] for at in range(8)]
    return (
        output,
        hidden_grad,
        small[0],
        small[1],
        projection_grad,
        jnp.stack([small[2], small[3]]),
        out_weight_grad,
        small[4],
        small[5],
        small[6],
        up_grad,
        sums[8 * width :],
        down_grad,
        small[7],
    )


def solution(mesh):
    placed = (
        P(("dp", "mp"), None),
        P("dp"),
        P(),
        P(),
        P(None, None, "mp"),
        P(None, "mp"),
        P("mp", None),
        P(),
        P(),
        P(),
        P(None, "mp"),
        P("mp"),
        P("mp", None),
        P(),
        P(("dp", "mp"), None),
    )
    return jax.shard_map(
        body,
        mesh=mesh,
        in_specs=placed,
        out_specs=(
            P(("dp", "mp"), None),
            P(("dp", "mp"), None),
            P(),
            P(),
            P("dp", None, "mp"),
            P(),
            P("mp", "dp"),
            P(),
            P(),
            P(),
            P("dp", "mp"),
            P(),
            P("mp", "dp"),
            P(),
        ),
        check_vma=False,
    )
```

```python
import functools

import jax
import jax.numpy as jnp
from jax import lax
from jax.experimental import pallas as pl
from jax.experimental.pallas import tpu as pltpu
from jax.sharding import PartitionSpec as P


HEAD_DIM = 64
TILE = 256
ROWS = 384
NEGATIVE = -1e30
EPS = 1e-05
LOW = jnp.bfloat16
WIDE = jnp.float32


def mm(left, right):
    return jnp.dot(left, right, preferred_element_type=WIDE)


def over_rows(left, right):
    return lax.dot_general(left, right, (((0,), (0,)), ((), ())), preferred_element_type=WIDE)


def over_cols(left, right):
    return lax.dot_general(left, right, (((1,), (1,)), ((), ())), preferred_element_type=WIDE)


def normalize(values):
    centered = values - jnp.mean(values, -1, keepdims=True)
    inverse = lax.rsqrt(jnp.mean(centered * centered, -1, keepdims=True) + EPS)
    return (centered * inverse, inverse)


def norm_back(incoming, scaled_in, inverse, gain):
    weighted = incoming * gain
    return inverse * (
        weighted
        - jnp.mean(weighted, -1, keepdims=True)
        - scaled_in * jnp.mean(weighted * scaled_in, -1, keepdims=True)
    )


def split_three(value):
    high = value.astype(LOW)
    rest = value - high.astype(WIDE)
    low = rest.astype(LOW)
    return high, low, (rest - low.astype(WIDE)).astype(LOW)


def in_vmem():
    return pl.BlockSpec(memory_space=pltpu.VMEM)


def in_smem():
    return pl.BlockSpec(memory_space=pltpu.SMEM)


def shaped(shape, kind):
    return jax.ShapeDtypeStruct(shape, kind)


def params(mebibytes=40):
    return pltpu.CompilerParams(vmem_limit_bytes=mebibytes << 20)


SHARD, CHIP, LENGTH, HOME = 0, 1, 2, 3


def offset(place_ref, slot, size):
    return pl.multiple_of((place_ref[SHARD] ^ slot) * size, size)


def open_kernel(blocks, place_ref, scale_ref, bias_ref, local_ref, out_ref, *refs):
    pieces, refs = refs[:blocks], refs[blocks:]
    members = (len(refs) - 4) // 2
    firsts, parts, (weights_ref, turned_ref, out_copy, sems) = refs[:members], refs[members : 2 * members], refs[2 * members :]
    size, part = pieces[0].shape[0], local_ref.shape[2]
    at_home = place_ref[HOME] == 1

    def copies(action):
        @pl.when(at_home)
        def _():
            for at in range(3):
                to = weights_ref.at[:, at * part : (at + 1) * part]
                getattr(pltpu.make_async_copy(local_ref.at[at], to, sems.at[0, at]), action)()
            getattr(pltpu.make_async_copy(out_ref, out_copy, sems.at[1, 0]), action)()

        @pl.when(jnp.logical_not(at_home))
        def _():
            for block, piece in enumerate(pieces):
                some = pl.ds(pl.multiple_of((place_ref[CHIP] ^ block) * size, size), size)
                getattr(pltpu.make_async_copy(piece.at[:, : 3 * part], weights_ref.at[some, :], sems.at[0, block]), action)()
                getattr(pltpu.make_async_copy(piece.at[:, 3 * part :], turned_ref.at[some, :], sems.at[1, block]), action)()

    copies("start")
    copies("wait")

    @pl.when(at_home)
    def _():
        turned_ref[...] = out_copy[...].T

    for first, out in zip(firsts, parts):
        out[...] = (mm(first[...], weights_ref[...]) * scale_ref[...] + bias_ref[...]).astype(LOW)


def open_up(place, local, out, scale, bias, pieces, firsts):
    rows, width = firsts[0].shape
    part = local.shape[2]
    anywhere = pl.BlockSpec(memory_space=pl.ANY)
    return pl.pallas_call(
        functools.partial(open_kernel, len(pieces)),
        in_specs=[in_smem()] + [in_vmem()] * 2 + [anywhere] * (2 + len(pieces)) + [in_vmem()] * len(firsts),
        out_specs=[in_vmem()] * (len(firsts) + 2),
        out_shape=[shaped((rows, 3 * part), LOW)] * len(firsts) + [shaped((width, 3 * part), LOW), shaped((width, part), LOW)],
        scratch_shapes=[pltpu.VMEM((part, width), LOW), pltpu.SemaphoreType.DMA((2, max(3, len(pieces))))],
        compiler_params=params(20),
        cost_estimate=pl.CostEstimate(flops=24 * rows * width * part, bytes_accessed=16 * width * part, transcendentals=0),
        name="open_up",
    )(place, scale, bias, local, out, *pieces, *firsts)


def attend_kernel(place_ref, *refs):
    members = (len(refs) - 6) // 2
    parts, refs = refs[:members], refs[members:]
    turned_ref, total_ref, outs = refs[0], refs[1], refs[2 : 2 + members]
    q_turned, v_turned, keys, keys_at, out_turned = refs[2 + members :]
    rows, width = keys.shape
    count = rows // members
    heads = width // HEAD_DIM
    length = place_ref[LENGTH]
    for slot, part in enumerate(parts):
        at = offset(place_ref, slot, count)
        q_turned[:, pl.ds(at, count)] = part[:, :width].T
        keys[pl.ds(at, count), :] = part[:, width : 2 * width]
        v_turned[:, pl.ds(at, count)] = part[:, 2 * width :].T
    key_row = lax.broadcasted_iota(jnp.int32, (rows, width), 0)
    lane = lax.broadcasted_iota(jnp.int32, (rows, width), 1)
    feature = lax.broadcasted_iota(jnp.int32, (width, TILE), 0)
    key_at = lax.broadcasted_iota(jnp.int32, (TILE, TILE), 0)
    query_at = lax.broadcasted_iota(jnp.int32, (TILE, TILE), 1)

    def one_head(head, _):
        first = pl.multiple_of(head * HEAD_DIM, HEAD_DIM)
        spare = lax.rem(head + 1, heads) * HEAD_DIM
        off = jnp.where(key_row < length, 0.0, NEGATIVE).astype(LOW)
        keys_at[...] = jnp.where(lane == spare, off, keys[...])
        for tile in range(rows // TILE):
            cols = slice(tile * TILE, (tile + 1) * TILE)
            upto = (tile + 1) * TILE
            query = q_turned[:, cols]
            query = jnp.where(feature // HEAD_DIM == head, query, jnp.where(feature == spare, 1.0, 0.0).astype(LOW))
            scores = mm(keys_at[:upto, :], query)
            last = jnp.where(key_at <= query_at, scores[tile * TILE :], NEGATIVE)
            highest = jnp.max(last, 0, keepdims=True)
            if tile:
                highest = jnp.maximum(highest, jnp.max(scores[: tile * TILE], 0, keepdims=True))
            weights = jnp.exp(last - highest)
            total = jnp.sum(weights, 0, keepdims=True)
            low = weights.astype(LOW)
            if tile:
                before = jnp.exp(scores[: tile * TILE] - highest)
                total = total + jnp.sum(before, 0, keepdims=True)
                low = jnp.concatenate([before.astype(LOW), low], 0)
            out = mm(v_turned[pl.ds(first, HEAD_DIM), :upto], low)
            out_turned[pl.ds(first, HEAD_DIM), cols] = out / total
            total_ref[pl.ds(head, 1), cols] = highest + jnp.log(total)
        return 0

    lax.fori_loop(0, heads, one_head, 0)
    turned_ref[...] = out_turned[...].astype(LOW)
    for slot, out in enumerate(outs):
        out[...] = out_turned[:, pl.ds(offset(place_ref, slot, count), count)].T.astype(LOW)


def attend(place, parts):
    members = len(parts)
    count, width = parts[0].shape[0], parts[0].shape[1] // 3
    rows = members * count
    return pl.pallas_call(
        attend_kernel,
        out_shape=[shaped((width, rows), LOW), shaped((8, rows), WIDE)] + [shaped((count, width), LOW)] * members,
        in_specs=[in_smem()] + [in_vmem()] * members,
        out_specs=[in_vmem()] * (2 + members),
        scratch_shapes=[
            pltpu.VMEM((width, rows), LOW),
            pltpu.VMEM((width, rows), LOW),
            pltpu.VMEM((rows, width), LOW),
            pltpu.VMEM((rows, width), LOW),
            pltpu.VMEM((width, rows), WIDE),
        ],
        compiler_params=params(),
        cost_estimate=pl.CostEstimate(flops=16 * rows * rows * width, bytes_accessed=8 * rows * width, transcendentals=rows * rows * 2),
        name="attend",
    )(place, *parts)


def attend_back_kernel(place_ref, *refs):
    members = (len(refs) - 17) // 2
    parts, grads, refs = refs[:members], refs[members : 2 * members], refs[2 * members :]
    turned_ref, total_ref, out_ref = refs[:3]
    (queries, keys, values, grad, q_turned, k_turned, g_turned, q_side, g_side, q_head, g_head, dq_turned, dk_sum, dv_sum) = refs[3:]
    rows, width = keys.shape
    count = rows // members
    heads = width // HEAD_DIM
    length = place_ref[LENGTH]
    for slot, (part, piece) in enumerate(zip(parts, grads)):
        at = offset(place_ref, slot, count)
        some = pl.ds(at, count)
        queries[some, :] = part[:, :width]
        keys[some, :] = part[:, width : 2 * width]
        values[some, :] = part[:, 2 * width :]
        grad[some, :] = piece[...]
        q_turned[:, some] = part[:, :width].T
        k_turned[:, some] = part[:, width : 2 * width].T
        g_turned[:, some] = piece[...].T
    dk_sum[...] = jnp.zeros_like(dk_sum)
    dv_sum[...] = jnp.zeros_like(dv_sum)
    lane_all = lax.broadcasted_iota(jnp.int32, (rows, width), 1)
    feature = lax.broadcasted_iota(jnp.int32, (width, rows), 0)
    lane = lax.broadcasted_iota(jnp.int32, (TILE, width), 1)
    key_at = lax.broadcasted_iota(jnp.int32, (TILE, TILE), 0)
    query_at = lax.broadcasted_iota(jnp.int32, (TILE, TILE), 1)
    none, one = jnp.zeros((), LOW), jnp.ones((), LOW)

    def one_head(head, _):
        first = pl.multiple_of(head * HEAD_DIM, HEAD_DIM)
        mine = pl.ds(first, HEAD_DIM)
        spare = lax.rem(head + 1, heads) * HEAD_DIM
        total = total_ref[pl.ds(head, 1), :]
        inner = jnp.sum(g_turned[mine, :].astype(WIDE) * turned_ref[mine, :].astype(WIDE), 0, keepdims=True)
        held = feature // HEAD_DIM == head

        def side(turned, taken, fourth):
            high, low, least = split_three(-taken)
            extra = jnp.where(feature == spare, high, jnp.where(feature == spare + 1, low, jnp.where(feature == spare + 2, least,
                jnp.where(feature == spare + 3, fourth, none))))
            return jnp.where(held, turned, extra)

        q_side[...] = side(q_turned[...], total, one)
        g_side[...] = side(g_turned[...], inner, none)
        own = lane_all // HEAD_DIM == head
        q_head[...] = jnp.where(own, queries[...], none)
        g_head[...] = jnp.where(own, grad[...], none)
        for tile in range(rows // TILE):
            start = tile * TILE
            at = slice(start, start + TILE)
            key_row = lax.broadcasted_iota(jnp.int32, (TILE, width), 0) + start
            off = jnp.where(key_row < length, 0.0, NEGATIVE).astype(LOW)
            ones = (lane >= spare) & (lane < spare + 3)
            scores = mm(jnp.where(ones, one, jnp.where(lane == spare + 3, off, keys[at, :])), q_side[:, start:])
            back = mm(jnp.where(ones, one, values[at, :]), g_side[:, start:])
            weights = jnp.exp(scores)
            near = jnp.where(key_at <= query_at, weights[:, :TILE], 0.0)
            weights = jnp.concatenate([near, weights[:, TILE:]], 1) if start + TILE < rows else near
            back_scores = (weights * back).astype(LOW)
            dv_sum[at, :] += mm(weights.astype(LOW), g_head[start:, :])
            dk_sum[at, :] += mm(back_scores, q_head[start:, :])
            dq = mm(k_turned[mine, at], back_scores)
            if tile:
                dq_turned[mine, start:] += dq
            else:
                dq_turned[mine, :] = dq
        return 0

    lax.fori_loop(0, heads, one_head, 0)
    for slot in range(members):
        some = pl.ds(offset(place_ref, slot, count), count)
        to = slice(slot * count, (slot + 1) * count)
        dq = dq_turned[:, some].T.astype(LOW).astype(WIDE)
        out_ref[to, :width] = (dq * HEAD_DIM**-0.5).astype(LOW)
        out_ref[to, width : 2 * width] = dk_sum[some, :].astype(LOW)
        out_ref[to, 2 * width :] = dv_sum[some, :].astype(LOW)


def attend_back(place, parts, grads, turned, total):
    members = len(parts)
    count, width = parts[0].shape[0], parts[0].shape[1] // 3
    rows = members * count
    low = lambda *shape: pltpu.VMEM(shape, LOW)
    wide = lambda *shape: pltpu.VMEM(shape, WIDE)
    return pl.pallas_call(
        attend_back_kernel,
        out_shape=shaped((rows, 3 * width), LOW),
        in_specs=[in_smem()] + [in_vmem()] * (2 * members + 2),
        out_specs=in_vmem(),
        scratch_shapes=[low(rows, width)] * 4 + [low(width, rows)] * 5 + [low(rows, width)] * 2
        + [wide(width, rows), wide(rows, width), wide(rows, width)],
        compiler_params=params(),
        cost_estimate=pl.CostEstimate(flops=40 * rows * rows * width, bytes_accessed=20 * rows * width, transcendentals=rows * rows * 2),
        name="attend_back",
    )(place, *parts, *grads, turned, total)


def project_kernel(*refs):
    members = (len(refs) - 6) // 2
    parts, outs, refs = refs[:members], refs[members : 2 * members], refs[2 * members :]
    hidden_ref, bias_ref, gain_ref, shift_ref, middle_ref, second_ref = refs
    total = hidden_ref[...].astype(WIDE) + bias_ref[...]
    for part, out in zip(parts, outs):
        total = total + over_cols(part[...], out[...])
    middle_ref[...] = total
    second_ref[...] = (normalize(total)[0] * gain_ref[...] + shift_ref[...]).astype(LOW)


def project(parts, outs, hidden, bias, gain, shift):
    rows, width = hidden.shape
    return pl.pallas_call(
        project_kernel,
        out_shape=[shaped((rows, width), WIDE), shaped((rows, width), LOW)],
        in_specs=[in_vmem()] * (2 * len(parts) + 4),
        out_specs=[in_vmem()] * 2,
        compiler_params=params(),
        cost_estimate=pl.CostEstimate(flops=2 * rows * width * width, bytes_accessed=2 * width * width + 10 * rows * width, transcendentals=rows),
        name="project",
    )(*parts, *outs, hidden, bias, gain, shift)


def feed_kernel(blocks, place_ref, x_one, x_two, g_one, g_two, bias_ref, up_local, down_local, *refs):
    pieces, refs = refs[:blocks], refs[blocks:]
    (act_ref, back_ref, sums_ref), outs, (up_ref, down_ref, up_sems, down_sems) = refs[:3], refs[3:7], refs[7:]
    half, size, hidden = x_one.shape[0], pieces[0].shape[0], up_ref.shape[1]
    at_home = place_ref[HOME] == 1

    def copies(action):
        @pl.when(at_home)
        def _():
            getattr(pltpu.make_async_copy(up_local, up_ref, up_sems.at[0]), action)()
            getattr(pltpu.make_async_copy(down_local, down_ref, down_sems.at[0]), action)()

        @pl.when(jnp.logical_not(at_home))
        def _():
            for block, piece in enumerate(pieces):
                some = pl.ds(pl.multiple_of((place_ref[CHIP] ^ block) * size, size), size)
                getattr(pltpu.make_async_copy(piece.at[:, :hidden], up_ref.at[some, :], up_sems.at[block]), action)()
                getattr(pltpu.make_async_copy(piece.at[:, hidden:], down_ref.at[some, :], down_sems.at[block]), action)()

    copies("start")
    copies("wait")
    sums = jnp.zeros(sums_ref.shape, WIDE)
    for which, (x_ref, g_ref) in enumerate(((x_one, g_one), (x_two, g_two))):
        for start in range(0, half, ROWS):
            at = slice(start, start + ROWS)
            to = slice(which * half + start, which * half + start + ROWS)
            before = mm(x_ref[at, :], up_ref[...]) + bias_ref[...]
            inside = 0.5 * (1.0 + lax.erf(before * 0.5**0.5))
            slope = inside + before * (jnp.exp(-0.5 * before * before) * (0.5 / jnp.pi) ** 0.5)
            act = (before * inside).astype(LOW)
            back = (over_cols(g_ref[at, :], down_ref[...]) * slope).astype(LOW)
            act_ref[to, :] = act
            back_ref[to, :] = back
            sums = sums + jnp.sum(back.astype(WIDE), 0, keepdims=True)
            outs[which][at, :] = mm(act, down_ref[...]).astype(outs[which].dtype)
            outs[2 + which][at, :] = over_cols(back, up_ref[...]).astype(outs[2 + which].dtype)
    sums_ref[...] = sums


def feed(place, x_one, x_two, g_one, g_two, bias, up, down, pieces, wide_first):
    half, width = x_one.shape
    hidden = up.shape[1]
    flat = [shaped((half, width), WIDE if wide_first else LOW), shaped((half, width), LOW)] * 2
    return pl.pallas_call(
        functools.partial(feed_kernel, len(pieces)),
        in_specs=[in_smem()] + [in_vmem()] * 5 + [pl.BlockSpec(memory_space=pl.ANY)] * (2 + len(pieces)),
        out_specs=[in_vmem()] * 7,
        out_shape=[shaped((2 * half, hidden), LOW)] * 2 + [shaped((1, hidden), WIDE)] + flat,
        scratch_shapes=[pltpu.VMEM((width, hidden), LOW), pltpu.VMEM((hidden, width), LOW)]
        + [pltpu.SemaphoreType.DMA((len(pieces),))] * 2,
        compiler_params=params(40),
        cost_estimate=pl.CostEstimate(flops=16 * half * width * hidden, bytes_accessed=4 * width * hidden, transcendentals=4 * half * hidden),
        name="feed",
    )(place, x_one, x_two, g_one, g_two, bias, up, down, *pieces)


def unproject_kernel(own_ref, mate_ref, near_ref, middle_ref, cotangent_ref, gain_ref, *refs):
    members = (len(refs) - 3) // 2
    weights, (low_ref, back_ref, sums_ref), outs = refs[:members], refs[members : members + 3], refs[members + 3 :]
    hat, inverse = normalize(middle_ref[...])
    second = own_ref[...] + mate_ref[...].astype(WIDE) + near_ref[...].astype(WIDE)
    cotangent = cotangent_ref[...].astype(WIDE)
    back = cotangent + norm_back(second, hat, inverse, gain_ref[...])
    low = back.astype(LOW)
    back_ref[...] = back
    low_ref[...] = low
    for weight, out in zip(weights, outs):
        out[...] = mm(low, weight[...]).astype(LOW)
    sums_ref[0:1, :] = jnp.sum(second * hat, 0, keepdims=True)
    sums_ref[1:2, :] = jnp.sum(second, 0, keepdims=True)
    sums_ref[2:3, :] = jnp.sum(back, 0, keepdims=True)
    sums_ref[3:4, :] = jnp.sum(cotangent, 0, keepdims=True)
    sums_ref[4:, :] = jnp.zeros_like(sums_ref[4:, :])


def unproject(own, mate, near, middle, cotangent, gain, outs):
    rows, width = own.shape
    members, part = len(outs), outs[0].shape[1]
    return pl.pallas_call(
        unproject_kernel,
        out_shape=[shaped((rows, width), LOW), shaped((rows, width), WIDE), shaped((8, width), WIDE)] + [shaped((rows, part), LOW)] * members,
        in_specs=[in_vmem()] * (6 + members),
        out_specs=[in_vmem()] * (3 + members),
        compiler_params=params(),
        cost_estimate=pl.CostEstimate(flops=2 * rows * width * width, bytes_accessed=2 * width * width + 18 * rows * width, transcendentals=rows),
        name="unproject",
    )(own, mate, near, middle, cotangent, gain, *outs)


def weigh_kernel(place_ref, *refs):
    pairs = (len(refs) - 6) // 6
    xs, gs, refs = refs[: 2 * pairs], refs[2 * pairs : 4 * pairs], refs[4 * pairs :]
    acts, backs, refs = refs[:pairs], refs[pairs : 2 * pairs], refs[2 * pairs :]
    up_keep, up_send, down_keep, down_send, x_turned, g_turned = refs
    count = xs[0].shape[0]
    blocks, size = 2 * up_keep.shape[0], up_keep.shape[1]
    for at, (x, g) in enumerate(zip(xs, gs)):
        x_turned[:, at * count : (at + 1) * count] = x[...].T
        g_turned[:, at * count : (at + 1) * count] = g[...].T
    for block in range(blocks):
        some = pl.ds(pl.multiple_of((place_ref[CHIP] ^ block) * size, size), size)
        product = lambda turned, parts: sum(mm(turned[some, at * 2 * count : (at + 1) * 2 * count], part[...]) for at, part in enumerate(parts))
        to = up_send if block % 2 else up_keep
        to[block // 2] = product(x_turned, backs).astype(LOW)
        to = down_send if block >= blocks // 2 else down_keep
        to[block % (blocks // 2)] = product(g_turned, acts).astype(LOW)


def weigh(place, xs, gs, acts, backs, chips):
    count, width = xs[0].shape
    hidden = acts[0].shape[1]
    rows = len(xs) * count
    return pl.pallas_call(
        weigh_kernel,
        in_specs=[in_smem()] + [in_vmem()] * (2 * len(xs) + 2 * len(acts)),
        out_specs=[in_vmem()] * 4,
        out_shape=[shaped((chips // 2, width // chips, hidden), LOW)] * 4,
        scratch_shapes=[pltpu.VMEM((width, rows), LOW)] * 2,
        compiler_params=params(56),
        cost_estimate=pl.CostEstimate(flops=4 * rows * width * hidden, bytes_accessed=4 * width * hidden + 8 * rows * width, transcendentals=0),
        name="weigh",
    )(place, *xs, *gs, *acts, *backs)


def turn_kernel(*refs):
    out = refs[-1]
    for at, ref in enumerate(refs[:-1]):
        count = ref.shape[0]
        out[:, at * count : (at + 1) * count] = ref[...].T


def turn(parts):
    count, width = parts[0].shape
    return pl.pallas_call(
        turn_kernel,
        in_specs=[in_vmem()] * len(parts),
        out_specs=in_vmem(),
        out_shape=shaped((width, len(parts) * count), LOW),
        compiler_params=params(20),
        cost_estimate=pl.CostEstimate(flops=0, bytes_accessed=4 * len(parts) * count * width, transcendentals=0),
        name="turn",
    )(*parts)


def weigh_late_kernel(place_ref, turned_ref, projected_ref, weight_ref, context_ref, *refs):
    members = len(refs) - 7
    lows, (one_keep, one_send, two_keep, two_send, gain_ref, sums_ref, out_turned) = refs[:members], refs[members:]
    count = lows[0].shape[0]
    blocks, size, cols = 2 * one_keep.shape[0], one_keep.shape[1], one_keep.shape[2]
    out = sum(mm(context_ref[:, pl.ds(offset(place_ref, slot, count), count)], low[...]) for slot, low in enumerate(lows))
    out_turned[...] = out.T.astype(LOW)
    sums = jnp.sum(projected_ref[...].astype(WIDE), 0, keepdims=True)
    sums_ref[...] = sums
    for block in range(blocks):
        some = pl.ds(pl.multiple_of((place_ref[CHIP] ^ block) * size, size), size)
        product = mm(turned_ref[some, :], projected_ref[...])
        weight = weight_ref[some, : product.shape[1]].astype(WIDE)
        gain = jnp.sum(product * weight, 1, keepdims=True)
        shift = jnp.sum(sums * weight, 1, keepdims=True)
        lane = lax.broadcasted_iota(jnp.int32, (size, gain_ref.shape[1]), 1)
        gain_ref[some, :] = jnp.where(lane == 0, gain, shift)
        to = one_send if block % 2 else one_keep
        to[block // 2] = product[:, :cols].astype(LOW)
        to = two_send if block >= blocks // 2 else two_keep
        rest = product.shape[1] - cols
        to[block % (blocks // 2), :, :rest] = product[:, cols:].astype(LOW)
        to[block % (blocks // 2), :, rest:] = out_turned[some, :]


def weigh_late(place, turned, projected, weight, context, lows, chips):
    width, rows = turned.shape
    part = context.shape[0]
    cols = 2 * part
    return pl.pallas_call(
        weigh_late_kernel,
        in_specs=[in_smem()] + [in_vmem()] * (4 + len(lows)),
        out_specs=[in_vmem()] * 6,
        out_shape=[shaped((chips // 2, width // chips, cols), LOW)] * 4 + [shaped((width, 128), WIDE), shaped((1, 3 * part), WIDE)],
        scratch_shapes=[pltpu.VMEM((width, part), LOW)],
        compiler_params=params(),
        cost_estimate=pl.CostEstimate(flops=8 * rows * width * part, bytes_accessed=4 * rows * width + 12 * width * part, transcendentals=0),
        name="weigh_late",
    )(place, turned, projected, weight, context, *lows)


def flip(size, bit):
    return [(at, at ^ bit) for at in range(size)]


def add_low(kept, taken):
    return (kept.astype(WIDE) + taken.astype(WIDE)).astype(LOW)


def add_up(values, axis):
    bit = 1
    while bit < lax.axis_size(axis):
        values = values + lax.ppermute(values, axis, flip(lax.axis_size(axis), bit))
        bit *= 2
    return values


def body(hidden, lengths, first_gain, first_shift, projection_in, query_value_bias, projection_out, out_bias,
         second_gain, second_shift, up_weight, up_bias, down_weight, down_bias, cotangent):
    rows, width = hidden.shape
    heads_width = projection_in.shape[2]
    hidden_width = up_weight.shape[1]
    groups, members = lax.axis_size("dp"), lax.axis_size("mp")
    group, member = lax.axis_index("dp"), lax.axis_index("mp")
    chips = groups // 2
    core, chip = group % 2, group // 2
    size = width // chips
    scale = HEAD_DIM ** (-0.5)
    at_home = core == member // 2
    shard = jnp.where(at_home, member, member ^ 2)
    both = ("dp", "mp")
    away = [(at * 2 + 1 - z // 2, z) for at in range(chips) for z in range(members)]
    spot = lambda dp, mp: dp * members + mp
    far_pairs = [(spot(d, z), spot(d ^ 1, z ^ 2)) for d, z in away]
    near_mate_pairs = [(spot(d, z), spot(d ^ 1, z ^ 1)) for d in range(groups) for z in range(members)]
    away_pairs = lambda bit: [(spot(d, z), spot(d ^ (2 * bit), z)) for d, z in away]
    far = lambda value: lax.ppermute(value, both, far_pairs)
    mate = lambda value: lax.ppermute(value, "dp", flip(groups, 1))
    near = lambda value: lax.ppermute(value, "mp", flip(members, 1))
    near_mate = lambda value: lax.ppermute(value, both, near_mate_pairs)
    cross = lambda value, bit: lax.ppermute(value, "dp", flip(groups, 2 * bit))
    moved = lambda value: jnp.where(at_home, value, far(value))
    block_of = lambda value, block: lax.dynamic_slice_in_dim(value, (chip ^ block) * size, size, 0)
    row = lambda vector: vector.reshape(1, -1)
    tie = lambda *values: lax.optimization_barrier(values)

    def spread(piece):
        return [piece] + [lax.ppermute(piece, both, away_pairs(block)) for block in range(1, chips)]

    def assembled(pieces, local):
        for block, piece in enumerate(pieces):
            piece = jnp.where(at_home, block_of(local, block), piece)
            local = lax.dynamic_update_slice_in_dim(local, piece, (chip ^ block) * size, 0)
        return local

    stream_blocks = lambda value, axis: lax.dynamic_slice_in_dim(value, chip * size, size, axis)
    first_piece = jnp.concatenate([stream_blocks(projection_in, 0).reshape(size, -1), stream_blocks(projection_out, 1).T], 1)
    notes = jnp.concatenate([query_value_bias.reshape(-1), up_bias.astype(WIDE), jnp.broadcast_to(lengths.astype(WIDE), (512,))])
    hidden_far, notes_far, *first_pieces = tie(far(hidden), far(notes.reshape(-1, 128)), *spread(far(first_piece)))
    hidden_own = jnp.where(at_home, hidden, hidden_far)
    notes = jnp.where(at_home, notes, notes_far.reshape(-1))
    qv_bias = notes[: 2 * heads_width].reshape(2, heads_width)
    up_bias_own = row(notes[2 * heads_width : 2 * heads_width + hidden_width])
    length = notes[-1].astype(jnp.int32)
    place = jnp.stack([shard, chip, length, at_home.astype(jnp.int32)]).astype(jnp.int32)
    first_hat, first_inverse = normalize(hidden_own.astype(WIDE))
    first_own = (first_hat * first_gain + first_shift).astype(LOW)
    zero = jnp.zeros((heads_width,), WIDE)
    bias_flat = row(jnp.concatenate([qv_bias[0] * scale, zero, qv_bias[1]]))
    scale_flat = row(jnp.concatenate([zero + scale, zero + 1.0, zero + 1.0]))

    second_piece = jnp.concatenate([stream_blocks(up_weight, 0), stream_blocks(down_weight, 0)], 1)
    second_piece, cotangent_sent, first_own = tie(second_piece, cotangent, first_own)
    cotangent_far = far(cotangent_sent)
    first_near, first_mate = tie(near(first_own), mate(first_own))
    second_piece, first_near = tie(second_piece, first_near)
    second_far = far(second_piece)
    firsts = [first_own, first_near, first_mate, mate(first_near)]
    *parts, weight_flat, out_own = open_up(
        place, projection_in.transpose(1, 0, 2), projection_out, scale_flat, bias_flat, first_pieces, firsts
    )

    parts[1], cotangent_far = tie(parts[1], cotangent_far)
    cotangent_own = jnp.where(at_home, cotangent, cotangent_far)
    cotangent_near, cotangent_mate = near(cotangent_own), mate(cotangent_own)
    out_near, out_mate = near(out_own), mate(out_own)
    turned, total, *context = attend(place, parts)
    context[1], context[2], context[3], out_near, out_mate, cotangent_mate, second_far = tie(
        context[1], context[2], context[3], out_near, out_mate, cotangent_mate, second_far
    )
    second_pieces = spread(second_far)

    exchange = (lambda value: value, near, mate, near_mate)
    context = [move(part) for move, part in zip(exchange, context)]
    context[1], context[2], context[3], out_last = tie(context[1], context[2], context[3], mate(out_near))
    outs = [out_own, out_near, out_mate, out_last]
    middle, second_own = project(context, outs, hidden_own, row(out_bias), row(second_gain), row(second_shift))

    second_mate, second_near = mate(second_own), near(second_own)
    second_mate, cotangent_near, *second_pieces = tie(second_mate, cotangent_near, *second_pieces)
    cotangent_last = mate(cotangent_near)
    fed_weights = (up_bias_own, up_weight, down_weight, second_pieces)
    act_one, back_one, bias_one, out_zero, out_two, grad_zero, grad_two = feed(
        place, second_own, second_mate, cotangent_own, cotangent_mate, *fed_weights, True
    )
    grad_two_got, out_two_got = mate(grad_two), mate(out_two)
    second_near, cotangent_last, act_one = tie(second_near, cotangent_last, act_one)
    second_last = mate(second_near)
    act_two, back_two, bias_two, out_one, out_three, grad_one, grad_three = feed(
        place, second_near, second_last, cotangent_near, cotangent_last, *fed_weights, False
    )
    grad_next = add_low(grad_one, mate(grad_three))
    grad_near = near(grad_next)
    out_three, grad_next = tie(out_three, grad_next)
    out_next = add_low(out_one, mate(out_three))
    out_near_sum = near(out_next)
    second_own, out_next = tie(second_own, out_next)
    up_keep, up_send, down_keep, down_send = weigh(
        place,
        [second_own, second_mate, second_near, second_last],
        [cotangent_own, cotangent_mate, cotangent_near, cotangent_last],
        [act_one, act_two],
        [back_one, back_two],
        chips,
    )
    grad_near, up_keep = tie(grad_near, up_keep)
    low_middle, back_middle, sums_part, *back_context = unproject(
        grad_zero, grad_two_got, grad_near, middle, cotangent_own, row(second_gain), outs
    )

    def start_halves(held, up_keep, up_send, down_keep, down_send):
        bit = 1
        while True:
            top = chips // 2 // bit
            up_got, down_got = cross(up_send, bit), cross(down_send, top)
            bit *= 2
            if bit == chips:
                return held, [up_keep, up_got, down_keep, down_got]
            held, up_got, down_got = tie(held, up_got, down_got)
            up_sum, down_sum = add_low(up_keep, up_got), add_low(down_keep, down_got)
            up_keep, up_send = up_sum[0::2], up_sum[1::2]
            down_keep, down_send = jnp.split(down_sum, 2, 0)
            held, up_send, down_send = tie(held, up_send, down_send)

    end_halves = lambda up_keep, up_got, down_keep, down_got: jnp.concatenate(
        [add_low(up_keep, up_got)[0], add_low(down_keep, down_got)[0]], 1
    )
    count = width // groups

    def settled(value, value_far):
        value = jnp.where(at_home, value, value_far)
        kept = lax.dynamic_slice_in_dim(value, core * count, count, 0).astype(WIDE)
        return kept + mate(lax.dynamic_slice_in_dim(value, (1 - core) * count, count, 0)).astype(WIDE)

    back_context = [move(part) for move, part in zip(exchange, back_context)]
    back_context[1], back_context[2], back_context[3], low_middle = tie(back_context[1], back_context[2], back_context[3], low_middle)
    first_turned = turn(firsts)
    output = (middle + out_zero + out_two_got.astype(WIDE) + out_near_sum.astype(WIDE) + down_bias).astype(LOW)
    back_context[1], first_turned, output = tie(back_context[1], first_turned, output)
    output_far, low_mate, low_near = far(output), mate(low_middle), near(low_middle)
    back_context[1], fed_halves = start_halves(back_context[1], up_keep, up_send, down_keep, down_send)
    back_projected = attend_back(place, parts, back_context, turned, total)
    back_projected, low_mate, low_near, output_far, fed_halves[1], fed_halves[3] = tie(
        back_projected, low_mate, low_near, output_far, fed_halves[1], fed_halves[3]
    )
    lows = [low_middle, low_near, low_mate, mate(low_near)]

    fed_sum = end_halves(*fed_halves)
    fed_sum, back_projected = tie(fed_sum, back_projected)
    fed_far = far(fed_sum)
    *late_parts, late_gains, projected_sums = weigh_late(place, first_turned, back_projected, weight_flat, turned, lows, chips)
    late_parts[0], back_projected = tie(late_parts[0], back_projected)
    share_high = over_cols(back_projected[2 * rows :], weight_flat).astype(LOW)
    share_high, back_projected = tie(share_high, back_projected)
    share_got, share_low = tie(mate(share_high), over_cols(back_projected[: 2 * rows], weight_flat))
    share_sum = share_low + share_got.astype(WIDE)
    share_near = near(share_sum[rows:].astype(LOW))
    placed = lambda value, whole: lax.dynamic_update_slice(jnp.zeros((whole,), WIDE), value, (shard * value.shape[0],))
    first_shift_grad = late_gains[:, 1]
    first_gain_grad = (late_gains[:, 0] - first_shift * first_shift_grad) / first_gain
    sums = [
        first_gain_grad,
        first_shift_grad,
        placed(projected_sums[0, :heads_width], width),
        placed(projected_sums[0, 2 * heads_width :], width),
        sums_part[:4].reshape(-1),
        placed((bias_one + bias_two)[0], members * hidden_width),
    ]
    sums, late_halves = start_halves(jnp.concatenate(sums).reshape(-1, 128), *late_parts)
    sums = add_up(sums, "dp")
    share_near, sums, fed_far, late_halves[1], late_halves[3] = tie(share_near, sums, fed_far, late_halves[1], late_halves[3])
    late_sum = end_halves(*late_halves)
    back_first = share_sum[:rows] + share_near.astype(WIDE)
    hidden_grad = (back_middle + norm_back(back_first, first_hat, first_inverse, first_gain)).astype(LOW)
    hidden_grad, late_sum = tie(hidden_grad, late_sum)
    late_far, hidden_grad_far = far(late_sum), far(hidden_grad)
    sums = add_up(sums, "mp").reshape(-1)
    fed_grad, late_grad = settled(fed_sum, fed_far), settled(late_sum, late_far)
    hidden_grad_out = jnp.where(at_home, hidden_grad, hidden_grad_far)
    output = jnp.where(at_home, output, output_far)

    small = [sums[at * width : (at + 1) * width] for at in range(8)]
    return (
        output,
        hidden_grad_out,
        small[0],
        small[1],
        late_grad[:, : 3 * heads_width].reshape(-1, 3, heads_width),
        sums[2 * width : 4 * width].reshape(2, width),
        late_grad[:, 3 * heads_width :].T,
        small[6],
        small[4],
        small[5],
        fed_grad[:, :hidden_width],
        sums[8 * width :],
        fed_grad[:, hidden_width:].T,
        small[7],
    )


def solution(mesh):
    placed = (
        P(("dp", "mp"), None),
        P("dp"),
        P(),
        P(),
        P(None, None, "mp"),
        P(None, "mp"),
        P("mp", None),
        P(),
        P(),
        P(),
        P(None, "mp"),
        P("mp"),
        P("mp", None),
        P(),
        P(("dp", "mp"), None),
    )
    return jax.shard_map(
        body,
        mesh=mesh,
        in_specs=placed,
        out_specs=(
            P(("dp", "mp"), None),
            P(("dp", "mp"), None),
            P(),
            P(),
            P("dp", None, "mp"),
            P(),
            P("mp", "dp"),
            P(),
            P(),
            P(),
            P("dp", "mp"),
            P(),
            P("mp", "dp"),
            P(),
        ),
        check_vma=False,
    )
```

```python
import functools

import jax
import jax.numpy as jnp
from jax import lax
from jax.experimental import pallas as pl
from jax.experimental.pallas import tpu as pltpu
from jax.sharding import PartitionSpec as P


HEAD_DIM = 64
TILE = 256
ROWS = 384
NEGATIVE = -1e30
EPS = 1e-05
LOW = jnp.bfloat16
WIDE = jnp.float32


def mm(left, right):
    return jnp.dot(left, right, preferred_element_type=WIDE)


def over_rows(left, right):
    return lax.dot_general(left, right, (((0,), (0,)), ((), ())), preferred_element_type=WIDE)


def over_cols(left, right):
    return lax.dot_general(left, right, (((1,), (1,)), ((), ())), preferred_element_type=WIDE)


def normalize(values):
    centered = values - jnp.mean(values, -1, keepdims=True)
    inverse = lax.rsqrt(jnp.mean(centered * centered, -1, keepdims=True) + EPS)
    return (centered * inverse, inverse)


def norm_back(incoming, scaled_in, inverse, gain):
    weighted = incoming * gain
    return inverse * (
        weighted
        - jnp.mean(weighted, -1, keepdims=True)
        - scaled_in * jnp.mean(weighted * scaled_in, -1, keepdims=True)
    )


def split_three(value):
    high = value.astype(LOW)
    rest = value - high.astype(WIDE)
    low = rest.astype(LOW)
    return high, low, (rest - low.astype(WIDE)).astype(LOW)


def in_vmem():
    return pl.BlockSpec(memory_space=pltpu.VMEM)


def in_smem():
    return pl.BlockSpec(memory_space=pltpu.SMEM)


def shaped(shape, kind):
    return jax.ShapeDtypeStruct(shape, kind)


def params(mebibytes=40):
    return pltpu.CompilerParams(vmem_limit_bytes=mebibytes << 20)


SHARD, CHIP, LENGTH, HOME = 0, 1, 2, 3


def offset(place_ref, slot, size):
    return pl.multiple_of((place_ref[SHARD] ^ slot) * size, size)


def open_kernel(blocks, place_ref, scale_ref, bias_ref, local_ref, out_ref, *refs):
    pieces, refs = refs[:blocks], refs[blocks:]
    members = (len(refs) - 4) // 2
    firsts, parts, (weights_ref, turned_ref, out_copy, sems) = refs[:members], refs[members : 2 * members], refs[2 * members :]
    size, part = pieces[0].shape[0], local_ref.shape[2]
    at_home = place_ref[HOME] == 1

    def copies(action):
        @pl.when(at_home)
        def _():
            for at in range(3):
                to = weights_ref.at[:, at * part : (at + 1) * part]
                getattr(pltpu.make_async_copy(local_ref.at[at], to, sems.at[0, at]), action)()
            getattr(pltpu.make_async_copy(out_ref, out_copy, sems.at[1, 0]), action)()

        @pl.when(jnp.logical_not(at_home))
        def _():
            for block, piece in enumerate(pieces):
                some = pl.ds(pl.multiple_of((place_ref[CHIP] ^ block) * size, size), size)
                getattr(pltpu.make_async_copy(piece.at[:, : 3 * part], weights_ref.at[some, :], sems.at[0, block]), action)()
                getattr(pltpu.make_async_copy(piece.at[:, 3 * part :], turned_ref.at[some, :], sems.at[1, block]), action)()

    copies("start")
    copies("wait")

    @pl.when(at_home)
    def _():
        turned_ref[...] = out_copy[...].T

    for first, out in zip(firsts, parts):
        out[...] = (mm(first[...], weights_ref[...]) * scale_ref[...] + bias_ref[...]).astype(LOW)


def open_up(place, local, out, scale, bias, pieces, firsts):
    rows, width = firsts[0].shape
    part = local.shape[2]
    anywhere = pl.BlockSpec(memory_space=pltpu.HBM)
    return pl.pallas_call(
        functools.partial(open_kernel, len(pieces)),
        in_specs=[in_smem()] + [in_vmem()] * 2 + [anywhere] * (2 + len(pieces)) + [in_vmem()] * len(firsts),
        out_specs=[in_vmem()] * (len(firsts) + 2),
        out_shape=[shaped((rows, 3 * part), LOW)] * len(firsts) + [shaped((width, 3 * part), LOW), shaped((width, part), LOW)],
        scratch_shapes=[pltpu.VMEM((part, width), LOW), pltpu.SemaphoreType.DMA((2, max(3, len(pieces))))],
        compiler_params=params(24),
        cost_estimate=pl.CostEstimate(flops=24 * rows * width * part, bytes_accessed=16 * width * part, transcendentals=0),
        name="open_up",
    )(place, scale, bias, local, out, *pieces, *firsts)


def attend_kernel(place_ref, *refs):
    members = (len(refs) - 6) // 2
    parts, refs = refs[:members], refs[members:]
    turned_ref, total_ref, outs = refs[0], refs[1], refs[2 : 2 + members]
    q_turned, v_turned, keys, keys_at, out_turned = refs[2 + members :]
    rows, width = keys.shape
    count = rows // members
    heads = width // HEAD_DIM
    length = place_ref[LENGTH]
    for slot, part in enumerate(parts):
        at = offset(place_ref, slot, count)
        q_turned[:, pl.ds(at, count)] = part[:, :width].T
        keys[pl.ds(at, count), :] = part[:, width : 2 * width]
        v_turned[:, pl.ds(at, count)] = part[:, 2 * width :].T
    key_row = lax.broadcasted_iota(jnp.int32, (rows, width), 0)
    lane = lax.broadcasted_iota(jnp.int32, (rows, width), 1)
    feature = lax.broadcasted_iota(jnp.int32, (width, TILE), 0)
    key_at = lax.broadcasted_iota(jnp.int32, (TILE, TILE), 0)
    query_at = lax.broadcasted_iota(jnp.int32, (TILE, TILE), 1)

    def one_head(head, _):
        first = pl.multiple_of(head * HEAD_DIM, HEAD_DIM)
        spare = lax.rem(head + 1, heads) * HEAD_DIM
        off = jnp.where(key_row < length, 0.0, NEGATIVE).astype(LOW)
        keys_at[...] = jnp.where(lane == spare, off, keys[...])

        def product(tile):
            query = q_turned[:, tile * TILE : (tile + 1) * TILE]
            query = jnp.where(feature // HEAD_DIM == head, query, jnp.where(feature == spare, 1.0, 0.0).astype(LOW))
            return mm(keys_at[: (tile + 1) * TILE, :], query)

        later = product(0)
        for tile in range(rows // TILE):
            cols = slice(tile * TILE, (tile + 1) * TILE)
            upto = (tile + 1) * TILE
            scores = later
            if upto < rows:
                later = product(tile + 1)
            last = jnp.where(key_at <= query_at, scores[tile * TILE :], NEGATIVE)
            highest = jnp.max(last, 0, keepdims=True)
            if tile:
                highest = jnp.maximum(highest, jnp.max(scores[: tile * TILE], 0, keepdims=True))
            weights = jnp.exp(last - highest)
            total = jnp.sum(weights, 0, keepdims=True)
            low = weights.astype(LOW)
            if tile:
                before = jnp.exp(scores[: tile * TILE] - highest)
                total = total + jnp.sum(before, 0, keepdims=True)
                low = jnp.concatenate([before.astype(LOW), low], 0)
            out = mm(v_turned[pl.ds(first, HEAD_DIM), :upto], low)
            out_turned[pl.ds(first, HEAD_DIM), cols] = out / total
            total_ref[pl.ds(head, 1), cols] = highest + jnp.log(total)
        return 0

    lax.fori_loop(0, heads, one_head, 0)
    turned_ref[...] = out_turned[...].astype(LOW)
    for slot, out in enumerate(outs):
        out[...] = out_turned[:, pl.ds(offset(place_ref, slot, count), count)].T.astype(LOW)


def attend(place, parts):
    members = len(parts)
    count, width = parts[0].shape[0], parts[0].shape[1] // 3
    rows = members * count
    return pl.pallas_call(
        attend_kernel,
        out_shape=[shaped((width, rows), LOW), shaped((8, rows), WIDE)] + [shaped((count, width), LOW)] * members,
        in_specs=[in_smem()] + [in_vmem()] * members,
        out_specs=[in_vmem()] * (2 + members),
        scratch_shapes=[
            pltpu.VMEM((width, rows), LOW),
            pltpu.VMEM((width, rows), LOW),
            pltpu.VMEM((rows, width), LOW),
            pltpu.VMEM((rows, width), LOW),
            pltpu.VMEM((width, rows), WIDE),
        ],
        compiler_params=params(32),
        cost_estimate=pl.CostEstimate(flops=16 * rows * rows * width, bytes_accessed=8 * rows * width, transcendentals=rows * rows * 2),
        name="attend",
    )(place, *parts)


def attend_back_kernel(place_ref, *refs):
    members = (len(refs) - 17) // 2
    parts, grads, refs = refs[:members], refs[members : 2 * members], refs[2 * members :]
    turned_ref, total_ref, out_ref = refs[:3]
    (queries, keys, values, grad, q_turned, k_turned, g_turned, q_side, g_side, q_head, g_head, dq_turned, dk_sum, dv_sum) = refs[3:]
    rows, width = keys.shape
    count = rows // members
    heads = width // HEAD_DIM
    length = place_ref[LENGTH]
    for slot, (part, piece) in enumerate(zip(parts, grads)):
        at = offset(place_ref, slot, count)
        some = pl.ds(at, count)
        queries[some, :] = part[:, :width]
        keys[some, :] = part[:, width : 2 * width]
        values[some, :] = part[:, 2 * width :]
        grad[some, :] = piece[...]
        q_turned[:, some] = part[:, :width].T
        k_turned[:, some] = part[:, width : 2 * width].T
        g_turned[:, some] = piece[...].T
    dk_sum[...] = jnp.zeros_like(dk_sum)
    dv_sum[...] = jnp.zeros_like(dv_sum)
    lane_all = lax.broadcasted_iota(jnp.int32, (rows, width), 1)
    feature = lax.broadcasted_iota(jnp.int32, (width, rows), 0)
    lane = lax.broadcasted_iota(jnp.int32, (TILE, width), 1)
    key_at = lax.broadcasted_iota(jnp.int32, (TILE, TILE), 0)
    query_at = lax.broadcasted_iota(jnp.int32, (TILE, TILE), 1)
    none, one = jnp.zeros((), LOW), jnp.ones((), LOW)

    def one_head(head, _):
        first = pl.multiple_of(head * HEAD_DIM, HEAD_DIM)
        mine = pl.ds(first, HEAD_DIM)
        spare = lax.rem(head + 1, heads) * HEAD_DIM
        total = total_ref[pl.ds(head, 1), :]
        inner = jnp.sum(g_turned[mine, :].astype(WIDE) * turned_ref[mine, :].astype(WIDE), 0, keepdims=True)
        held = feature // HEAD_DIM == head

        def side(turned, taken, fourth):
            high, low, least = split_three(-taken)
            extra = jnp.where(feature == spare, high, jnp.where(feature == spare + 1, low, jnp.where(feature == spare + 2, least,
                jnp.where(feature == spare + 3, fourth, none))))
            return jnp.where(held, turned, extra)

        q_side[...] = side(q_turned[...], total, one)
        g_side[...] = side(g_turned[...], inner, none)
        own = lane_all // HEAD_DIM == head
        q_head[...] = jnp.where(own, queries[...], none)
        g_head[...] = jnp.where(own, grad[...], none)

        def products(start):
            at = slice(start, start + TILE)
            key_row = lax.broadcasted_iota(jnp.int32, (TILE, width), 0) + start
            off = jnp.where(key_row < length, 0.0, NEGATIVE).astype(LOW)
            ones = (lane >= spare) & (lane < spare + 3)
            scores = mm(jnp.where(ones, one, jnp.where(lane == spare + 3, off, keys[at, :])), q_side[:, start:])
            return scores, mm(jnp.where(ones, one, values[at, :]), g_side[:, start:])

        later = products(0)
        for tile in range(rows // TILE):
            start = tile * TILE
            at = slice(start, start + TILE)
            scores, back = later
            if start + TILE < rows:
                later = products(start + TILE)
            weights = jnp.exp(scores)
            near = jnp.where(key_at <= query_at, weights[:, :TILE], 0.0)
            weights = jnp.concatenate([near, weights[:, TILE:]], 1) if start + TILE < rows else near
            back_scores = (weights * back).astype(LOW)
            dv_sum[at, :] += mm(weights.astype(LOW), g_head[start:, :])
            dk_sum[at, :] += mm(back_scores, q_head[start:, :])
            dq = mm(k_turned[mine, at], back_scores)
            if tile:
                dq_turned[mine, start:] += dq
            else:
                dq_turned[mine, :] = dq
        return 0

    lax.fori_loop(0, heads, one_head, 0)
    for slot in range(members):
        some = pl.ds(offset(place_ref, slot, count), count)
        to = slice(slot * count, (slot + 1) * count)
        dq = dq_turned[:, some].T.astype(LOW).astype(WIDE)
        out_ref[to, :width] = (dq * HEAD_DIM**-0.5).astype(LOW)
        out_ref[to, width : 2 * width] = dk_sum[some, :].astype(LOW)
        out_ref[to, 2 * width :] = dv_sum[some, :].astype(LOW)


def attend_back(place, parts, grads, turned, total):
    members = len(parts)
    count, width = parts[0].shape[0], parts[0].shape[1] // 3
    rows = members * count
    low = lambda *shape: pltpu.VMEM(shape, LOW)
    wide = lambda *shape: pltpu.VMEM(shape, WIDE)
    return pl.pallas_call(
        attend_back_kernel,
        out_shape=shaped((rows, 3 * width), LOW),
        in_specs=[in_smem()] + [in_vmem()] * (2 * members + 2),
        out_specs=in_vmem(),
        scratch_shapes=[low(rows, width)] * 4 + [low(width, rows)] * 5 + [low(rows, width)] * 2
        + [wide(width, rows), wide(rows, width), wide(rows, width)],
        compiler_params=params(40),
        cost_estimate=pl.CostEstimate(flops=40 * rows * rows * width, bytes_accessed=20 * rows * width, transcendentals=rows * rows * 2),
        name="attend_back",
    )(place, *parts, *grads, turned, total)


def project_kernel(*refs):
    members = (len(refs) - 6) // 2
    parts, outs, refs = refs[:members], refs[members : 2 * members], refs[2 * members :]
    hidden_ref, bias_ref, gain_ref, shift_ref, middle_ref, second_ref = refs
    total = hidden_ref[...].astype(WIDE) + bias_ref[...]
    for part, out in zip(parts, outs):
        total = total + over_cols(part[...], out[...])
    middle_ref[...] = total
    second_ref[...] = (normalize(total)[0] * gain_ref[...] + shift_ref[...]).astype(LOW)


def project(parts, outs, hidden, bias, gain, shift):
    rows, width = hidden.shape
    return pl.pallas_call(
        project_kernel,
        out_shape=[shaped((rows, width), WIDE), shaped((rows, width), LOW)],
        in_specs=[in_vmem()] * (2 * len(parts) + 4),
        out_specs=[in_vmem()] * 2,
        compiler_params=params(24),
        cost_estimate=pl.CostEstimate(flops=2 * rows * width * width, bytes_accessed=2 * width * width + 10 * rows * width, transcendentals=rows),
        name="project",
    )(*parts, *outs, hidden, bias, gain, shift)


def feed_kernel(blocks, place_ref, x_one, x_two, g_one, g_two, bias_ref, up_local, down_local, *refs):
    pieces, refs = refs[:blocks], refs[blocks:]
    act_ref, back_ref, sums_ref, out_ref, grad_ref, other_ref, up_ref, down_ref, up_sems, down_sems = refs
    half, size = x_one.shape[0], pieces[0].shape[0] // 2
    at_home = place_ref[HOME] == 1

    def copies(action):
        @pl.when(at_home)
        def _():
            getattr(pltpu.make_async_copy(up_local, up_ref, up_sems.at[0]), action)()
            getattr(pltpu.make_async_copy(down_local, down_ref, down_sems.at[0]), action)()

        @pl.when(jnp.logical_not(at_home))
        def _():
            for block, piece in enumerate(pieces):
                some = pl.ds(pl.multiple_of((place_ref[CHIP] ^ block) * size, size), size)
                getattr(pltpu.make_async_copy(piece.at[:size, :], up_ref.at[some, :], up_sems.at[block]), action)()
                getattr(pltpu.make_async_copy(piece.at[size:, :], down_ref.at[some, :], down_sems.at[block]), action)()

    copies("start")
    copies("wait")
    sums = jnp.zeros(sums_ref.shape, WIDE)
    for which, (x_ref, g_ref) in enumerate(((x_one, g_one), (x_two, g_two))):
        for start in range(0, half, ROWS):
            at = slice(start, start + ROWS)
            to = slice(which * half + start, which * half + start + ROWS)
            before = mm(x_ref[at, :], up_ref[...]) + bias_ref[...]
            inside = 0.5 * (1.0 + lax.erf(before * 0.5**0.5))
            slope = inside + before * (jnp.exp(-0.5 * before * before) * (0.5 / jnp.pi) ** 0.5)
            act = (before * inside).astype(LOW)
            back = (over_cols(g_ref[at, :], down_ref[...]) * slope).astype(LOW)
            act_ref[to, :] = act
            back_ref[to, :] = back
            sums = sums + jnp.sum(back.astype(WIDE), 0, keepdims=True)
            out, grad = mm(act, down_ref[...]), over_cols(back, up_ref[...])
            if which:
                other_ref[at, :] = out.astype(LOW)
                other_ref[half + start : half + start + ROWS, :] = grad.astype(LOW)
            else:
                out_ref[at, :] = out.astype(out_ref.dtype)
                grad_ref[at, :] = grad.astype(grad_ref.dtype)
    sums_ref[...] = sums


def feed(place, x_one, x_two, g_one, g_two, bias, up, down, pieces, wide_first):
    half, width = x_one.shape
    hidden = up.shape[1]
    flat = [shaped((half, width), WIDE if wide_first else LOW)] * 2 + [shaped((2 * half, width), LOW)]
    return pl.pallas_call(
        functools.partial(feed_kernel, len(pieces)),
        in_specs=[in_smem()] + [in_vmem()] * 5 + [pl.BlockSpec(memory_space=pltpu.HBM)] * (2 + len(pieces)),
        out_specs=[in_vmem()] * 6,
        out_shape=[shaped((2 * half, hidden), LOW)] * 2 + [shaped((1, hidden), WIDE)] + flat,
        scratch_shapes=[pltpu.VMEM((width, hidden), LOW), pltpu.VMEM((hidden, width), LOW)]
        + [pltpu.SemaphoreType.DMA((len(pieces),))] * 2,
        compiler_params=params(40),
        cost_estimate=pl.CostEstimate(flops=16 * half * width * hidden, bytes_accessed=4 * width * hidden, transcendentals=4 * half * hidden),
        name="feed",
    )(place, x_one, x_two, g_one, g_two, bias, up, down, *pieces)


def unproject_kernel(own_ref, mate_ref, near_ref, middle_ref, cotangent_ref, gain_ref, *refs):
    members = (len(refs) - 3) // 2
    weights, (low_ref, back_ref, sums_ref), outs = refs[:members], refs[members : members + 3], refs[members + 3 :]
    hat, inverse = normalize(middle_ref[...])
    second = own_ref[...] + mate_ref[own_ref.shape[0] :, :].astype(WIDE) + near_ref[...].astype(WIDE)
    cotangent = cotangent_ref[...].astype(WIDE)
    back = cotangent + norm_back(second, hat, inverse, gain_ref[...])
    low = back.astype(LOW)
    back_ref[...] = back
    low_ref[...] = low
    for weight, out in zip(weights, outs):
        out[...] = mm(low, weight[...]).astype(LOW)
    sums_ref[0:1, :] = jnp.sum(second * hat, 0, keepdims=True)
    sums_ref[1:2, :] = jnp.sum(second, 0, keepdims=True)
    sums_ref[2:3, :] = jnp.sum(back, 0, keepdims=True)
    sums_ref[3:4, :] = jnp.sum(cotangent, 0, keepdims=True)
    sums_ref[4:, :] = jnp.zeros_like(sums_ref[4:, :])


def unproject(own, mate, near, middle, cotangent, gain, outs):
    rows, width = own.shape
    members, part = len(outs), outs[0].shape[1]
    return pl.pallas_call(
        unproject_kernel,
        out_shape=[shaped((rows, width), LOW), shaped((rows, width), WIDE), shaped((8, width), WIDE)] + [shaped((rows, part), LOW)] * members,
        in_specs=[in_vmem()] * (6 + members),
        out_specs=[in_vmem()] * (3 + members),
        compiler_params=params(56),
        cost_estimate=pl.CostEstimate(flops=2 * rows * width * width, bytes_accessed=2 * width * width + 18 * rows * width, transcendentals=rows),
        name="unproject",
    )(own, mate, near, middle, cotangent, gain, *outs)


def weigh_kernel(place_ref, *refs):
    pairs = (len(refs) - 6) // 6
    xs, gs, refs = refs[: 2 * pairs], refs[2 * pairs : 4 * pairs], refs[4 * pairs :]
    acts, backs, refs = refs[:pairs], refs[pairs : 2 * pairs], refs[2 * pairs :]
    up_keep, up_send, down_keep, down_send, x_turned, g_turned = refs
    count = xs[0].shape[0]
    blocks, size = 2 * up_keep.shape[0], up_keep.shape[1]
    for at, (x, g) in enumerate(zip(xs, gs)):
        x_turned[:, at * count : (at + 1) * count] = x[...].T
        g_turned[:, at * count : (at + 1) * count] = g[...].T
    for block in range(blocks):
        some = pl.ds(pl.multiple_of((place_ref[CHIP] ^ block) * size, size), size)
        product = lambda turned, parts: sum(mm(turned[some, at * 2 * count : (at + 1) * 2 * count], part[...]) for at, part in enumerate(parts))
        to = up_send if block % 2 else up_keep
        to[block // 2] = product(x_turned, backs).astype(LOW)
        to = down_send if block >= blocks // 2 else down_keep
        to[block % (blocks // 2)] = product(g_turned, acts).astype(LOW)


def weigh(place, xs, gs, acts, backs, chips):
    count, width = xs[0].shape
    hidden = acts[0].shape[1]
    rows = len(xs) * count
    return pl.pallas_call(
        weigh_kernel,
        in_specs=[in_smem()] + [in_vmem()] * (2 * len(xs) + 2 * len(acts)),
        out_specs=[in_vmem()] * 4,
        out_shape=[shaped((chips // 2, width // chips, hidden), LOW)] * 4,
        scratch_shapes=[pltpu.VMEM((width, rows), LOW)] * 2,
        compiler_params=params(40),
        cost_estimate=pl.CostEstimate(flops=4 * rows * width * hidden, bytes_accessed=4 * width * hidden + 8 * rows * width, transcendentals=0),
        name="weigh",
    )(place, *xs, *gs, *acts, *backs)


def turn_kernel(*refs):
    out = refs[-1]
    for at, ref in enumerate(refs[:-1]):
        count = ref.shape[0]
        out[:, at * count : (at + 1) * count] = ref[...].T


def turn(parts):
    count, width = parts[0].shape
    return pl.pallas_call(
        turn_kernel,
        in_specs=[in_vmem()] * len(parts),
        out_specs=in_vmem(),
        out_shape=shaped((width, len(parts) * count), LOW),
        compiler_params=params(40),
        cost_estimate=pl.CostEstimate(flops=0, bytes_accessed=4 * len(parts) * count * width, transcendentals=0),
        name="turn",
    )(*parts)


def weigh_late_kernel(place_ref, turned_ref, projected_ref, weight_ref, context_ref, *refs):
    members = len(refs) - 7
    lows, (one_keep, one_send, two_keep, two_send, gain_ref, sums_ref, out_turned) = refs[:members], refs[members:]
    count = lows[0].shape[0]
    blocks, size, cols = 2 * one_keep.shape[0], one_keep.shape[1], one_keep.shape[2]
    out = sum(mm(context_ref[:, pl.ds(offset(place_ref, slot, count), count)], low[...]) for slot, low in enumerate(lows))
    out_turned[...] = out.T.astype(LOW)
    sums = jnp.sum(projected_ref[...].astype(WIDE), 0, keepdims=True)
    sums_ref[...] = sums
    for block in range(blocks):
        some = pl.ds(pl.multiple_of((place_ref[CHIP] ^ block) * size, size), size)
        product = mm(turned_ref[some, :], projected_ref[...])
        weight = weight_ref[some, : product.shape[1]].astype(WIDE)
        gain = jnp.sum(product * weight, 1, keepdims=True)
        shift = jnp.sum(sums * weight, 1, keepdims=True)
        lane = lax.broadcasted_iota(jnp.int32, (size, gain_ref.shape[1]), 1)
        gain_ref[some, :] = jnp.where(lane == 0, gain, shift)
        to = one_send if block % 2 else one_keep
        to[block // 2] = product[:, :cols].astype(LOW)
        to = two_send if block >= blocks // 2 else two_keep
        rest = product.shape[1] - cols
        to[block % (blocks // 2), :, :rest] = product[:, cols:].astype(LOW)
        to[block % (blocks // 2), :, rest:] = out_turned[some, :]


def weigh_late(place, turned, projected, weight, context, lows, chips):
    width, rows = turned.shape
    part = context.shape[0]
    cols = 2 * part
    return pl.pallas_call(
        weigh_late_kernel,
        in_specs=[in_smem()] + [in_vmem()] * (4 + len(lows)),
        out_specs=[in_vmem()] * 6,
        out_shape=[shaped((chips // 2, width // chips, cols), LOW)] * 4
        + [shaped((width, 128), WIDE), shaped((1, 3 * part), WIDE)],
        scratch_shapes=[pltpu.VMEM((width, part), LOW)],
        compiler_params=params(32),
        cost_estimate=pl.CostEstimate(flops=8 * rows * width * part, bytes_accessed=4 * rows * width + 12 * width * part, transcendentals=0),
        name="weigh_late",
    )(place, turned, projected, weight, context, *lows)


def share_kernel(projected_ref, weight_ref, zero_ref, one_ref, high_ref):
    count = zero_ref.shape[0]
    high_ref[...] = over_cols(projected_ref[2 * count :, :], weight_ref[...]).astype(LOW)
    one_ref[...] = over_cols(projected_ref[count : 2 * count, :], weight_ref[...]).astype(LOW)
    zero_ref[...] = over_cols(projected_ref[:count, :], weight_ref[...])


def share(projected, weight):
    rows, width = projected.shape[0], weight.shape[0]
    return pl.pallas_call(
        share_kernel,
        in_specs=[in_vmem()] * 2,
        out_specs=[in_vmem()] * 3,
        out_shape=[shaped((rows // 4, width), WIDE), shaped((rows // 4, width), LOW), shaped((rows // 2, width), LOW)],
        compiler_params=params(40),
        cost_estimate=pl.CostEstimate(flops=2 * rows * width * weight.shape[1], bytes_accessed=6 * rows * width, transcendentals=0),
        name="share",
    )(projected, weight)


def flip(size, bit):
    return [(at, at ^ bit) for at in range(size)]


def add_low(kept, taken):
    return (kept.astype(WIDE) + taken.astype(WIDE)).astype(LOW)


def add_up(values, axis, wide):
    size, bit = lax.axis_size(axis), 1
    while bit < size:
        mate = lax.ppermute(values, axis, flip(size, bit))
        if wide and 2 * bit < size:
            values = (values + mate) + (lax.ppermute(values, axis, flip(size, 2 * bit)) + lax.ppermute(values, axis, flip(size, 3 * bit)))
            bit *= 2
        else:
            values = values + mate
        bit *= 2
    return values

PLAN = {'first': (None, 1), 'notes': (None, 0), 'cotangent': (3, 6), 'second': (None, 3), 'pieces': (None, 2), 'outs': (None, 4), 'seconds': (None, 70), 'last': (None, 5), 'cotmate': (None, 7), 'cotnear': (None, 8), 'secnear': (None, 8), 'two': (11, 12), 'three': (11, None), 'fed': (None, 15), 'out': (None, 14), 'low': (None, 16), 'fedrest': (None, 16), 'hand': (None, 20), 'output': (None, 16), 'late': (None, 20), 'laterest': (None, 21), 'latehand': (None, None), 'early': 1, 'half': 1, 'sums': 19, 'middle': 20, 'wide': 0, 'lateend': 1}


class Box:
    def __init__(self, value=None, at=None):
        self.value, self.at = value, at


class Order:
    def __init__(self):
        self.boxes, self.later = [], {}

    def keep(self, value, at):
        box = Box(value, at)
        self.boxes.append(box)
        return box

    def point(self, at, *values):
        boxes = [box for box in self.boxes if box.at == at]
        if boxes:
            tied = lax.optimization_barrier((*values, *[box.value for box in boxes]))
            values = tied[: len(values)]
            for box, value in zip(boxes, tied[len(values) :]):
                box.value, box.at = value, None
        for action in self.later.pop(at, ()):
            action()
        return values if len(values) > 1 else values[0]

    def send(self, name, operand, move):
        start, end = PLAN[name]
        result = Box()

        def go():
            with jax.named_scope(name):
                result.value = move(operand.value)
            result.at = end
            self.boxes.append(result)

        if start is None:
            go()
        else:
            operand.at = start
            if operand not in self.boxes:
                self.boxes.append(operand)
            self.later.setdefault(start, []).append(go)
        return result


def body(hidden, lengths, first_gain, first_shift, projection_in, query_value_bias, projection_out, out_bias,
         second_gain, second_shift, up_weight, up_bias, down_weight, down_bias, cotangent):
    rows, width = hidden.shape
    heads_width = projection_in.shape[2]
    hidden_width = up_weight.shape[1]
    groups, members = lax.axis_size("dp"), lax.axis_size("mp")
    group, member = lax.axis_index("dp"), lax.axis_index("mp")
    chips = groups // 2
    core, chip = group % 2, group // 2
    size, count = width // chips, width // groups
    scale = HEAD_DIM ** (-0.5)
    at_home = core == member // 2
    shard = jnp.where(at_home, member, member ^ 2)
    both = ("dp", "mp")
    away = [(at * 2 + 1 - z // 2, z) for at in range(chips) for z in range(members)]
    spot = lambda dp, mp: dp * members + mp
    far_pairs = [(spot(d, z), spot(d ^ 1, z ^ 2)) for d, z in away]
    near_mate_pairs = [(spot(d, z), spot(d ^ 1, z ^ 1)) for d in range(groups) for z in range(members)]
    hand_pairs = [(spot(d, z), spot(d, z ^ 2)) for d, z in away] + [(spot(d ^ 1, z), spot(d, z)) for d, z in away]
    away_pairs = lambda bit: [(spot(d, z), spot(d ^ (2 * bit), z)) for d, z in away]
    far = lambda value: lax.ppermute(value, both, far_pairs)
    mate = lambda value: lax.ppermute(value, "dp", flip(groups, 1))
    near = lambda value: lax.ppermute(value, "mp", flip(members, 1))
    near_mate = lambda value: lax.ppermute(value, both, near_mate_pairs)
    cross = lambda bit: lambda value: lax.ppermute(value, "dp", flip(groups, 2 * bit))
    row = lambda vector: vector.reshape(1, -1)
    order = Order()
    keep, point, send = order.keep, order.point, order.send
    pick = lambda own, got: jnp.where(at_home, own, got)

    def spread(name, piece):
        return [piece] + [send(name, keep(piece.value, None), lambda value, block=block: lax.ppermute(value, both, away_pairs(block))) for block in range(1, chips)]

    block_of = lambda value, axis: lax.dynamic_slice_in_dim(value, chip * size, size, axis)
    first_piece = jnp.concatenate([block_of(projection_in, 0).reshape(size, -1), block_of(projection_out, 1).T], 1)
    notes = jnp.concatenate([query_value_bias.reshape(-1), up_bias.astype(WIDE), jnp.broadcast_to(lengths.astype(WIDE), (512,))])
    first_far = send("first", keep(first_piece, None), far)
    notes_far = send("notes", keep(notes.reshape(-1, 128), None), far)
    cotangent_far = send("cotangent", keep(cotangent, None), far)
    second_piece = jnp.concatenate([block_of(up_weight, 0), block_of(down_weight, 0)], 0)
    second_far = send("second", keep(second_piece, None), far)
    hidden_own = pick(hidden, point(0, far(hidden)))
    notes = pick(notes, notes_far.value.reshape(-1))
    qv_bias = notes[: 2 * heads_width].reshape(2, heads_width)
    up_bias_own = row(notes[2 * heads_width : 2 * heads_width + hidden_width])
    length = notes[-1].astype(jnp.int32)
    place = jnp.stack([shard, chip, length, at_home.astype(jnp.int32)]).astype(jnp.int32)
    first_hat, first_inverse = normalize(hidden_own.astype(WIDE))
    first_own = (first_hat * first_gain + first_shift).astype(LOW)
    zero = jnp.zeros((heads_width,), WIDE)
    bias_flat = row(jnp.concatenate([qv_bias[0] * scale, zero, qv_bias[1]]))
    scale_flat = row(jnp.concatenate([zero + scale, zero + 1.0, zero + 1.0]))

    first_own = point(1, first_own)
    first_pieces = spread("pieces", first_far)
    first_near, first_mate = point(2, near(first_own), mate(first_own))
    firsts = [first_own, first_near, first_mate, mate(first_near)]
    *parts, weight_flat, out_own = open_up(
        place, projection_in.transpose(1, 0, 2), projection_out, scale_flat, bias_flat, [piece.value for piece in first_pieces], firsts
    )

    parts[1], out_own = point(3, parts[1], out_own)
    out_near, out_mate = send("outs", keep(out_own, None), near), send("outs", keep(out_own, None), mate)
    out_own = out_own
    turned, total, *context = attend(place, parts)
    context[1], context[2], context[3] = point(4, context[1], context[2], context[3])
    if second_far.value is not None:
        second_pieces = spread("seconds", second_far)
    out_last = send("last", keep(out_near.value, None), mate)
    exchange = (lambda value: value, near, mate, near_mate)
    context = [move(part) for move, part in zip(exchange, context)]
    context[1], context[2], context[3] = point(5, context[1], context[2], context[3])
    outs = [out_own, out_near.value, out_mate.value, out_last.value]
    middle, second_own = project(context, outs, hidden_own, row(out_bias), row(second_gain), row(second_shift))

    second_own = point(6, second_own)
    cotangent_own = keep(pick(cotangent, cotangent_far.value), None)
    second_mate, cotangent_mate, second_own, cotangent_own.value = point(
        7, mate(second_own), mate(cotangent_own.value), second_own, cotangent_own.value
    )
    second_near = send("secnear", keep(second_own, None), near)
    cotangent_near = send("cotnear", keep(cotangent_own.value, None), near)
    second_mate = point(70, second_mate)
    fed_weights = (up_bias_own, up_weight, down_weight, [piece.value for piece in second_pieces])
    act_one, back_one, bias_one, out_zero, grad_zero, other_two = feed(
        place, second_own, second_mate, cotangent_own.value, cotangent_mate, *fed_weights, True
    )
    act_one, other_two = point(8, act_one, other_two)
    two_got = send("two", keep(other_two, None), mate)
    second_near.value, cotangent_near.value = point(9, second_near.value, cotangent_near.value)
    second_last, cotangent_last = mate(second_near.value), mate(cotangent_near.value)
    act_two, back_two, bias_two, out_one, grad_one, other_three = feed(
        place, second_near.value, second_last, cotangent_near.value, cotangent_last, *fed_weights, False
    )
    three_got = mate(point(10, other_three))
    grad_next = add_low(grad_one, three_got[rows:])
    grad_near = near(grad_next)
    second_keep, grad_next = point(11, second_own, grad_next)
    up_keep, up_send, down_keep, down_send = weigh(
        place,
        [second_keep, second_mate, second_near.value, second_last],
        [cotangent_own.value, cotangent_mate, cotangent_near.value, cotangent_last],
        [act_one, act_two],
        [back_one, back_two],
        chips,
    )
    up_got = send("fed", keep(up_send, None), cross(1))
    down_got = send("fed", keep(down_send, None), cross(chips // 2))
    grad_near, up_keep = point(12, grad_near, up_keep)
    low_middle, back_middle, sums_part, *back_context = unproject(
        grad_zero, two_got.value, grad_near, middle, cotangent_own.value, row(second_gain), outs
    )
    out_next = add_low(out_one, three_got[:rows])
    out_sum = send("out", keep(out_next, None), near)

    back_context[1], low_middle = point(13, back_context[1], low_middle)
    back_context = [move(part) for move, part in zip(exchange, back_context)]
    first_turned = keep(turn(firsts), 14)
    back_context[1], back_context[2], back_context[3], low_middle = point(14, back_context[1], back_context[2], back_context[3], low_middle)

    def halved(up_keep, up_got, down_keep, down_got):
        return add_low(up_keep, up_got), add_low(down_keep, down_got)

    def handed(name, value):
        rows_of = lambda at: lax.dynamic_slice_in_dim(value, at * count, count, 0)
        kept, given = rows_of(member // 2), rows_of(1 - member // 2)
        return kept, send(name, keep(kept, None), far), send(name, keep(given, None), lambda value: lax.ppermute(value, both, hand_pairs))

    settled = lambda kept, got_far, got: pick(kept, got_far.value).astype(WIDE) + got.value.astype(WIDE)
    low_mate, low_near = send("low", keep(low_middle, None), mate), send("low", keep(low_middle, None), near)
    written = lambda: (middle + out_zero + two_got.value[:rows].astype(WIDE) + out_sum.value.astype(WIDE) + down_bias).astype(LOW)
    if PLAN["early"]:
        output = keep(written(), 15)
    back_context[1], up_keep, down_keep = point(15, back_context[1], up_keep, down_keep)
    up_sum, down_sum = halved(up_keep, up_got.value, down_keep, down_got.value) if PLAN["half"] else (None, None)

    def rest(up_sum, down_sum, name):
        bit, sent = 2, []
        while bit < chips:
            half = down_sum.shape[0] // 2
            sent = send(name, keep(up_sum[1::2], None), cross(bit)), send(name, keep(down_sum[half:], None), cross(chips // 2 // bit))
            bit *= 2
            if bit < chips:
                up_sum, down_sum = halved(up_sum[0::2], sent[0].value, down_sum[:half], sent[1].value)
        return up_sum[0::2], sent[0], down_sum[: down_sum.shape[0] // 2], sent[1]

    def finish(up_keep, up_got, down_keep, down_got):
        up_sum, down_sum = halved(up_keep, up_got.value, down_keep, down_got.value)
        return jnp.concatenate([up_sum[0], down_sum[0]], 1)

    if PLAN["half"]:
        fed_rest = rest(up_sum, down_sum, "fedrest")
    if PLAN["early"]:
        output_far = send("output", keep(output.value, None), far)
    back_projected = attend_back(place, parts, back_context, turned, total)
    back_projected = point(16, back_projected)
    lows = [low_middle, low_near.value, low_mate.value, mate(low_near.value)]

    if not PLAN["half"]:
        up_sum, down_sum = halved(up_keep, up_got.value, down_keep, down_got.value)
        up_sum, back_projected = lax.optimization_barrier((up_sum, back_projected))
        fed_rest = rest(up_sum, down_sum, "fedrest")
    if PLAN["half"]:
        fed_sum = finish(*fed_rest)
        fed_sum, back_projected = lax.optimization_barrier((fed_sum, back_projected))
        fed_parts = handed("hand", fed_sum)
    share_zero, share_one, share_high = share(back_projected, weight_flat)
    share_high, back_projected = point(17, share_high, back_projected)
    share_got = mate(share_high)
    share_zero, share_next, back_projected = point(
        18, share_zero + share_got[:rows].astype(WIDE), add_low(share_one, share_got[rows:]), back_projected
    )
    share_near = near(share_next)
    *late_parts, late_gains, projected_sums = weigh_late(place, first_turned.value, back_projected, weight_flat, turned, lows, chips)
    late_parts[1], late_parts[3], share_zero = point(19, late_parts[1], late_parts[3], share_zero)
    late_up, late_down = send("late", keep(late_parts[1], None), cross(1)), send("late", keep(late_parts[3], None), cross(chips // 2))
    gains = keep(late_gains, PLAN["sums"])
    if not PLAN["early"]:
        output_far = send("output", keep(written(), None), far)
    if not PLAN["half"]:
        fed_parts = handed("hand", finish(*fed_rest))

    def gather_sums():
        placed = lambda value, whole: lax.dynamic_update_slice(jnp.zeros((whole,), WIDE), value, (shard * value.shape[0],))
        shift_grad = gains.value[:, 1]
        sums = [
            (gains.value[:, 0] - first_shift * shift_grad) / first_gain,
            shift_grad,
            placed(projected_sums[0, :heads_width], width),
            placed(projected_sums[0, 2 * heads_width :], width),
            sums_part[:4].reshape(-1),
            placed((bias_one + bias_two)[0], members * hidden_width),
        ]
        return add_up(jnp.concatenate(sums).reshape(-1, 128), "dp", PLAN["wide"])

    if PLAN["sums"] != 20:
        sums = keep(gather_sums(), PLAN["middle"])
    share_near, share_zero = point(20, share_near, share_zero)
    if PLAN["sums"] == 20:
        sums = keep(gather_sums(), PLAN["middle"])
    late_rest = rest(*halved(late_parts[0], late_up.value, late_parts[2], late_down.value), "laterest")
    if PLAN["lateend"] == 0:
        late_end = handed("latehand", finish(*late_rest))
    back_first = share_zero + share_near.astype(WIDE)
    hidden_grad = (back_middle + norm_back(back_first, first_hat, first_inverse, first_gain)).astype(LOW)
    hidden_grad = point(21, hidden_grad)
    hidden_grad_far = far(hidden_grad)
    if PLAN["lateend"] == 1:
        late_end = handed("latehand", finish(*late_rest))
    sums = add_up(sums.value, "mp", PLAN["wide"]).reshape(-1)
    fed_grad, late_grad = settled(*fed_parts), settled(*late_end)
    small = [sums[at * width : (at + 1) * width] for at in range(8)]
    return (
        pick(output.value if PLAN["early"] else written(), output_far.value),
        pick(hidden_grad, hidden_grad_far),
        small[0],
        small[1],
        late_grad[:, : 3 * heads_width].reshape(-1, 3, heads_width),
        sums[2 * width : 4 * width].reshape(2, width),
        late_grad[:, 3 * heads_width :].T,
        small[6],
        small[4],
        small[5],
        fed_grad[:, :hidden_width],
        sums[8 * width :],
        fed_grad[:, hidden_width:].T,
        small[7],
    )


def solution(mesh):
    placed = (
        P(("dp", "mp"), None),
        P("dp"),
        P(),
        P(),
        P(None, None, "mp"),
        P(None, "mp"),
        P("mp", None),
        P(),
        P(),
        P(),
        P(None, "mp"),
        P("mp"),
        P("mp", None),
        P(),
        P(("dp", "mp"), None),
    )
    return jax.shard_map(
        body,
        mesh=mesh,
        in_specs=placed,
        out_specs=(
            P(("dp", "mp"), None),
            P(("dp", "mp"), None),
            P(),
            P(),
            P("dp", None, "mp"),
            P(),
            P("mp", "dp"),
            P(),
            P(),
            P(),
            P("dp", "mp"),
            P(),
            P("mp", "dp"),
            P(),
        ),
        check_vma=False,
    )
```

```python
import functools

import jax
import jax.numpy as jnp
from jax import lax
from jax.experimental import pallas as pl
from jax.experimental.pallas import tpu as pltpu
from jax.sharding import PartitionSpec as P


HEAD_DIM = 64
TILE = 256
ROWS = 384
NEGATIVE = -1e30
EPS = 1e-05
LOW = jnp.bfloat16
WIDE = jnp.float32


def mm(left, right):
    return jnp.dot(left, right, preferred_element_type=WIDE)


def over_rows(left, right):
    return lax.dot_general(left, right, (((0,), (0,)), ((), ())), preferred_element_type=WIDE)


def over_cols(left, right):
    return lax.dot_general(left, right, (((1,), (1,)), ((), ())), preferred_element_type=WIDE)


def normalize(values):
    centered = values - jnp.mean(values, -1, keepdims=True)
    inverse = lax.rsqrt(jnp.mean(centered * centered, -1, keepdims=True) + EPS)
    return (centered * inverse, inverse)


def norm_back(incoming, scaled_in, inverse, gain):
    weighted = incoming * gain
    return inverse * (
        weighted
        - jnp.mean(weighted, -1, keepdims=True)
        - scaled_in * jnp.mean(weighted * scaled_in, -1, keepdims=True)
    )


def split_three(value):
    high = value.astype(LOW)
    rest = value - high.astype(WIDE)
    low = rest.astype(LOW)
    return high, low, (rest - low.astype(WIDE)).astype(LOW)


def in_vmem():
    return pl.BlockSpec(memory_space=pltpu.VMEM)


def in_smem():
    return pl.BlockSpec(memory_space=pltpu.SMEM)


def shaped(shape, kind):
    return jax.ShapeDtypeStruct(shape, kind)


def params(mebibytes=40):
    return pltpu.CompilerParams(vmem_limit_bytes=mebibytes << 20)


SHARD, CHIP, LENGTH, HOME = 0, 1, 2, 3


def offset(place_ref, slot, size):
    return pl.multiple_of((place_ref[SHARD] ^ slot) * size, size)


def open_kernel(blocks, place_ref, scale_ref, bias_ref, local_ref, out_ref, *refs):
    pieces, refs = refs[:blocks], refs[blocks:]
    members = (len(refs) - 4) // 2
    firsts, parts, (weights_ref, turned_ref, out_copy, sems) = refs[:members], refs[members : 2 * members], refs[2 * members :]
    size, part = pieces[0].shape[0], local_ref.shape[2]
    at_home = place_ref[HOME] == 1

    def copies(action):
        @pl.when(at_home)
        def _():
            for at in range(3):
                to = weights_ref.at[:, at * part : (at + 1) * part]
                getattr(pltpu.make_async_copy(local_ref.at[at], to, sems.at[0, at]), action)()
            getattr(pltpu.make_async_copy(out_ref, out_copy, sems.at[1, 0]), action)()

        @pl.when(jnp.logical_not(at_home))
        def _():
            for block, piece in enumerate(pieces):
                some = pl.ds(pl.multiple_of((place_ref[CHIP] ^ block) * size, size), size)
                getattr(pltpu.make_async_copy(piece.at[:, : 3 * part], weights_ref.at[some, :], sems.at[0, block]), action)()
                getattr(pltpu.make_async_copy(piece.at[:, 3 * part :], turned_ref.at[some, :], sems.at[1, block]), action)()

    copies("start")
    copies("wait")

    @pl.when(at_home)
    def _():
        turned_ref[...] = out_copy[...].T

    for first, out in zip(firsts, parts):
        out[...] = (mm(first[...], weights_ref[...]) * scale_ref[...] + bias_ref[...]).astype(LOW)


def open_up(place, local, out, scale, bias, pieces, firsts):
    rows, width = firsts[0].shape
    part = local.shape[2]
    anywhere = pl.BlockSpec(memory_space=pltpu.HBM)
    return pl.pallas_call(
        functools.partial(open_kernel, len(pieces)),
        in_specs=[in_smem()] + [in_vmem()] * 2 + [anywhere] * (2 + len(pieces)) + [in_vmem()] * len(firsts),
        out_specs=[in_vmem()] * (len(firsts) + 2),
        out_shape=[shaped((rows, 3 * part), LOW)] * len(firsts) + [shaped((width, 3 * part), LOW), shaped((width, part), LOW)],
        scratch_shapes=[pltpu.VMEM((part, width), LOW), pltpu.SemaphoreType.DMA((2, max(3, len(pieces))))],
        compiler_params=params(24),
        cost_estimate=pl.CostEstimate(flops=24 * rows * width * part, bytes_accessed=16 * width * part, transcendentals=0),
        name="open_up",
    )(place, scale, bias, local, out, *pieces, *firsts)


def attend_kernel(place_ref, *refs):
    members = (len(refs) - 6) // 2
    parts, refs = refs[:members], refs[members:]
    turned_ref, total_ref, outs = refs[0], refs[1], refs[2 : 2 + members]
    q_turned, v_turned, keys, keys_at, out_turned = refs[2 + members :]
    rows, width = keys.shape
    count = rows // members
    heads = width // HEAD_DIM
    length = place_ref[LENGTH]
    for slot, part in enumerate(parts):
        at = offset(place_ref, slot, count)
        q_turned[:, pl.ds(at, count)] = part[:, :width].T
        keys[pl.ds(at, count), :] = part[:, width : 2 * width]
        v_turned[:, pl.ds(at, count)] = part[:, 2 * width :].T
    key_row = lax.broadcasted_iota(jnp.int32, (rows, width), 0)
    lane = lax.broadcasted_iota(jnp.int32, (rows, width), 1)
    feature = lax.broadcasted_iota(jnp.int32, (width, TILE), 0)
    key_at = lax.broadcasted_iota(jnp.int32, (TILE, TILE), 0)
    query_at = lax.broadcasted_iota(jnp.int32, (TILE, TILE), 1)

    def one_head(head, _):
        first = pl.multiple_of(head * HEAD_DIM, HEAD_DIM)
        spare = lax.rem(head + 1, heads) * HEAD_DIM
        off = jnp.where(key_row < length, 0.0, NEGATIVE).astype(LOW)
        keys_at[...] = jnp.where(lane == spare, off, keys[...])

        def product(tile):
            query = q_turned[:, tile * TILE : (tile + 1) * TILE]
            query = jnp.where(feature // HEAD_DIM == head, query, jnp.where(feature == spare, 1.0, 0.0).astype(LOW))
            return mm(keys_at[: (tile + 1) * TILE, :], query)

        later = product(0)
        for tile in range(rows // TILE):
            cols = slice(tile * TILE, (tile + 1) * TILE)
            upto = (tile + 1) * TILE
            scores = later
            if upto < rows:
                later = product(tile + 1)
            last = jnp.where(key_at <= query_at, scores[tile * TILE :], NEGATIVE)
            highest = jnp.max(last, 0, keepdims=True)
            if tile:
                highest = jnp.maximum(highest, jnp.max(scores[: tile * TILE], 0, keepdims=True))
            weights = jnp.exp(last - highest)
            total = jnp.sum(weights, 0, keepdims=True)
            low = weights.astype(LOW)
            if tile:
                before = jnp.exp(scores[: tile * TILE] - highest)
                total = total + jnp.sum(before, 0, keepdims=True)
                low = jnp.concatenate([before.astype(LOW), low], 0)
            out = mm(v_turned[pl.ds(first, HEAD_DIM), :upto], low)
            out_turned[pl.ds(first, HEAD_DIM), cols] = out / total
            total_ref[pl.ds(head, 1), cols] = highest + jnp.log(total)
        return 0

    lax.fori_loop(0, heads, one_head, 0)
    turned_ref[...] = out_turned[...].astype(LOW)
    for slot, out in enumerate(outs):
        out[...] = out_turned[:, pl.ds(offset(place_ref, slot, count), count)].T.astype(LOW)


def attend(place, parts):
    members = len(parts)
    count, width = parts[0].shape[0], parts[0].shape[1] // 3
    rows = members * count
    return pl.pallas_call(
        attend_kernel,
        out_shape=[shaped((width, rows), LOW), shaped((8, rows), WIDE)] + [shaped((count, width), LOW)] * members,
        in_specs=[in_smem()] + [in_vmem()] * members,
        out_specs=[in_vmem()] * (2 + members),
        scratch_shapes=[
            pltpu.VMEM((width, rows), LOW),
            pltpu.VMEM((width, rows), LOW),
            pltpu.VMEM((rows, width), LOW),
            pltpu.VMEM((rows, width), LOW),
            pltpu.VMEM((width, rows), WIDE),
        ],
        compiler_params=params(32),
        cost_estimate=pl.CostEstimate(flops=16 * rows * rows * width, bytes_accessed=8 * rows * width, transcendentals=rows * rows * 2),
        name="attend",
    )(place, *parts)


def attend_back_kernel(place_ref, *refs):
    members = (len(refs) - 17) // 2
    parts, grads, refs = refs[:members], refs[members : 2 * members], refs[2 * members :]
    turned_ref, total_ref, out_ref = refs[:3]
    (queries, keys, values, grad, q_turned, k_turned, g_turned, q_side, g_side, q_head, g_head, dq_turned, dk_sum, dv_sum) = refs[3:]
    rows, width = keys.shape
    count = rows // members
    heads = width // HEAD_DIM
    length = place_ref[LENGTH]
    for slot, (part, piece) in enumerate(zip(parts, grads)):
        at = offset(place_ref, slot, count)
        some = pl.ds(at, count)
        queries[some, :] = part[:, :width]
        keys[some, :] = part[:, width : 2 * width]
        values[some, :] = part[:, 2 * width :]
        grad[some, :] = piece[...]
        q_turned[:, some] = part[:, :width].T
        k_turned[:, some] = part[:, width : 2 * width].T
        g_turned[:, some] = piece[...].T
    dk_sum[...] = jnp.zeros_like(dk_sum)
    dv_sum[...] = jnp.zeros_like(dv_sum)
    lane_all = lax.broadcasted_iota(jnp.int32, (rows, width), 1)
    feature = lax.broadcasted_iota(jnp.int32, (width, rows), 0)
    lane = lax.broadcasted_iota(jnp.int32, (TILE, width), 1)
    key_at = lax.broadcasted_iota(jnp.int32, (TILE, TILE), 0)
    query_at = lax.broadcasted_iota(jnp.int32, (TILE, TILE), 1)
    none, one = jnp.zeros((), LOW), jnp.ones((), LOW)

    def one_head(head, _):
        first = pl.multiple_of(head * HEAD_DIM, HEAD_DIM)
        mine = pl.ds(first, HEAD_DIM)
        spare = lax.rem(head + 1, heads) * HEAD_DIM
        total = total_ref[pl.ds(head, 1), :]
        inner = jnp.sum(g_turned[mine, :].astype(WIDE) * turned_ref[mine, :].astype(WIDE), 0, keepdims=True)
        held = feature // HEAD_DIM == head

        def side(turned, taken, fourth):
            high, low, least = split_three(-taken)
            extra = jnp.where(feature == spare, high, jnp.where(feature == spare + 1, low, jnp.where(feature == spare + 2, least,
                jnp.where(feature == spare + 3, fourth, none))))
            return jnp.where(held, turned, extra)

        q_side[...] = side(q_turned[...], total, one)
        g_side[...] = side(g_turned[...], inner, none)
        own = lane_all // HEAD_DIM == head
        q_head[...] = jnp.where(own, queries[...], none)
        g_head[...] = jnp.where(own, grad[...], none)

        def products(start):
            at = slice(start, start + TILE)
            key_row = lax.broadcasted_iota(jnp.int32, (TILE, width), 0) + start
            off = jnp.where(key_row < length, 0.0, NEGATIVE).astype(LOW)
            ones = (lane >= spare) & (lane < spare + 3)
            scores = mm(jnp.where(ones, one, jnp.where(lane == spare + 3, off, keys[at, :])), q_side[:, start:])
            return scores, mm(jnp.where(ones, one, values[at, :]), g_side[:, start:])

        later = products(0)
        for tile in range(rows // TILE):
            start = tile * TILE
            at = slice(start, start + TILE)
            scores, back = later
            if start + TILE < rows:
                later = products(start + TILE)
            weights = jnp.exp(scores)
            near = jnp.where(key_at <= query_at, weights[:, :TILE], 0.0)
            weights = jnp.concatenate([near, weights[:, TILE:]], 1) if start + TILE < rows else near
            back_scores = (weights * back).astype(LOW)
            dv_sum[at, :] += mm(weights.astype(LOW), g_head[start:, :])
            dk_sum[at, :] += mm(back_scores, q_head[start:, :])
            dq = mm(k_turned[mine, at], back_scores)
            if tile:
                dq_turned[mine, start:] += dq
            else:
                dq_turned[mine, :] = dq
        return 0

    lax.fori_loop(0, heads, one_head, 0)
    for slot in range(members):
        some = pl.ds(offset(place_ref, slot, count), count)
        to = slice(slot * count, (slot + 1) * count)
        dq = dq_turned[:, some].T.astype(LOW).astype(WIDE)
        out_ref[to, :width] = (dq * HEAD_DIM**-0.5).astype(LOW)
        out_ref[to, width : 2 * width] = dk_sum[some, :].astype(LOW)
        out_ref[to, 2 * width :] = dv_sum[some, :].astype(LOW)


def attend_back(place, parts, grads, turned, total):
    members = len(parts)
    count, width = parts[0].shape[0], parts[0].shape[1] // 3
    rows = members * count
    low = lambda *shape: pltpu.VMEM(shape, LOW)
    wide = lambda *shape: pltpu.VMEM(shape, WIDE)
    return pl.pallas_call(
        attend_back_kernel,
        out_shape=shaped((rows, 3 * width), LOW),
        in_specs=[in_smem()] + [in_vmem()] * (2 * members + 2),
        out_specs=in_vmem(),
        scratch_shapes=[low(rows, width)] * 4 + [low(width, rows)] * 5 + [low(rows, width)] * 2
        + [wide(width, rows), wide(rows, width), wide(rows, width)],
        compiler_params=params(40),
        cost_estimate=pl.CostEstimate(flops=40 * rows * rows * width, bytes_accessed=20 * rows * width, transcendentals=rows * rows * 2),
        name="attend_back",
    )(place, *parts, *grads, turned, total)


def project_kernel(*refs):
    members = (len(refs) - 6) // 2
    parts, outs, refs = refs[:members], refs[members : 2 * members], refs[2 * members :]
    hidden_ref, bias_ref, gain_ref, shift_ref, middle_ref, second_ref = refs
    total = hidden_ref[...].astype(WIDE) + bias_ref[...]
    for part, out in zip(parts, outs):
        total = total + over_cols(part[...], out[...])
    middle_ref[...] = total
    second_ref[...] = (normalize(total)[0] * gain_ref[...] + shift_ref[...]).astype(LOW)


def project(parts, outs, hidden, bias, gain, shift):
    rows, width = hidden.shape
    return pl.pallas_call(
        project_kernel,
        out_shape=[shaped((rows, width), WIDE), shaped((rows, width), LOW)],
        in_specs=[in_vmem()] * (2 * len(parts) + 4),
        out_specs=[in_vmem()] * 2,
        compiler_params=params(24),
        cost_estimate=pl.CostEstimate(flops=2 * rows * width * width, bytes_accessed=2 * width * width + 10 * rows * width, transcendentals=rows),
        name="project",
    )(*parts, *outs, hidden, bias, gain, shift)


def feed_kernel(blocks, place_ref, x_one, x_two, g_one, g_two, bias_ref, up_local, down_local, *refs):
    pieces, refs = refs[:blocks], refs[blocks:]
    act_ref, back_ref, sums_ref, out_ref, grad_ref, other_ref, up_ref, down_ref, up_sems, down_sems = refs
    half, size = x_one.shape[0], pieces[0].shape[0] // 2
    at_home = place_ref[HOME] == 1

    def copies(action):
        @pl.when(at_home)
        def _():
            getattr(pltpu.make_async_copy(up_local, up_ref, up_sems.at[0]), action)()
            getattr(pltpu.make_async_copy(down_local, down_ref, down_sems.at[0]), action)()

        @pl.when(jnp.logical_not(at_home))
        def _():
            for block, piece in enumerate(pieces):
                some = pl.ds(pl.multiple_of((place_ref[CHIP] ^ block) * size, size), size)
                getattr(pltpu.make_async_copy(piece.at[:size, :], up_ref.at[some, :], up_sems.at[block]), action)()
                getattr(pltpu.make_async_copy(piece.at[size:, :], down_ref.at[some, :], down_sems.at[block]), action)()

    copies("start")
    copies("wait")
    sums = jnp.zeros(sums_ref.shape, WIDE)
    for which, (x_ref, g_ref) in enumerate(((x_one, g_one), (x_two, g_two))):
        for start in range(0, half, ROWS):
            at = slice(start, start + ROWS)
            to = slice(which * half + start, which * half + start + ROWS)
            before = mm(x_ref[at, :], up_ref[...]) + bias_ref[...]
            inside = 0.5 * (1.0 + lax.erf(before * 0.5**0.5))
            slope = inside + before * (jnp.exp(-0.5 * before * before) * (0.5 / jnp.pi) ** 0.5)
            act = (before * inside).astype(LOW)
            back = (over_cols(g_ref[at, :], down_ref[...]) * slope).astype(LOW)
            act_ref[to, :] = act
            back_ref[to, :] = back
            sums = sums + jnp.sum(back.astype(WIDE), 0, keepdims=True)
            out, grad = mm(act, down_ref[...]), over_cols(back, up_ref[...])
            if which:
                other_ref[at, :] = out.astype(LOW)
                other_ref[half + start : half + start + ROWS, :] = grad.astype(LOW)
            else:
                out_ref[at, :] = out.astype(out_ref.dtype)
                grad_ref[at, :] = grad.astype(grad_ref.dtype)
    sums_ref[...] = sums


def feed(place, x_one, x_two, g_one, g_two, bias, up, down, pieces, wide_first):
    half, width = x_one.shape
    hidden = up.shape[1]
    flat = [shaped((half, width), WIDE if wide_first else LOW)] * 2 + [shaped((2 * half, width), LOW)]
    return pl.pallas_call(
        functools.partial(feed_kernel, len(pieces)),
        in_specs=[in_smem()] + [in_vmem()] * 5 + [pl.BlockSpec(memory_space=pltpu.HBM)] * (2 + len(pieces)),
        out_specs=[in_vmem()] * 6,
        out_shape=[shaped((2 * half, hidden), LOW)] * 2 + [shaped((1, hidden), WIDE)] + flat,
        scratch_shapes=[pltpu.VMEM((width, hidden), LOW), pltpu.VMEM((hidden, width), LOW)]
        + [pltpu.SemaphoreType.DMA((len(pieces),))] * 2,
        compiler_params=params(40),
        cost_estimate=pl.CostEstimate(flops=16 * half * width * hidden, bytes_accessed=4 * width * hidden, transcendentals=4 * half * hidden),
        name="feed",
    )(place, x_one, x_two, g_one, g_two, bias, up, down, *pieces)


def unproject_kernel(own_ref, mate_ref, near_ref, middle_ref, cotangent_ref, gain_ref, *refs):
    members = (len(refs) - 3) // 2
    weights, (low_ref, back_ref, sums_ref), outs = refs[:members], refs[members : members + 3], refs[members + 3 :]
    hat, inverse = normalize(middle_ref[...])
    second = own_ref[...] + mate_ref[own_ref.shape[0] :, :].astype(WIDE) + near_ref[...].astype(WIDE)
    cotangent = cotangent_ref[...].astype(WIDE)
    back = cotangent + norm_back(second, hat, inverse, gain_ref[...])
    low = back.astype(LOW)
    back_ref[...] = back
    low_ref[...] = low
    for weight, out in zip(weights, outs):
        out[...] = mm(low, weight[...]).astype(LOW)
    sums_ref[0:1, :] = jnp.sum(second * hat, 0, keepdims=True)
    sums_ref[1:2, :] = jnp.sum(second, 0, keepdims=True)
    sums_ref[2:3, :] = jnp.sum(back, 0, keepdims=True)
    sums_ref[3:4, :] = jnp.sum(cotangent, 0, keepdims=True)
    sums_ref[4:, :] = jnp.zeros_like(sums_ref[4:, :])


def unproject(own, mate, near, middle, cotangent, gain, outs):
    rows, width = own.shape
    members, part = len(outs), outs[0].shape[1]
    return pl.pallas_call(
        unproject_kernel,
        out_shape=[shaped((rows, width), LOW), shaped((rows, width), WIDE), shaped((8, width), WIDE)] + [shaped((rows, part), LOW)] * members,
        in_specs=[in_vmem()] * (6 + members),
        out_specs=[in_vmem()] * (3 + members),
        compiler_params=params(24),
        cost_estimate=pl.CostEstimate(flops=2 * rows * width * width, bytes_accessed=2 * width * width + 18 * rows * width, transcendentals=rows),
        name="unproject",
    )(own, mate, near, middle, cotangent, gain, *outs)


def weigh_kernel(place_ref, *refs):
    pairs = (len(refs) - 6) // 6
    xs, gs, refs = refs[: 2 * pairs], refs[2 * pairs : 4 * pairs], refs[4 * pairs :]
    acts, backs, refs = refs[:pairs], refs[pairs : 2 * pairs], refs[2 * pairs :]
    up_keep, up_send, down_keep, down_send, x_turned, g_turned = refs
    count = xs[0].shape[0]
    blocks, size = 2 * up_keep.shape[0], up_keep.shape[1]
    for at, (x, g) in enumerate(zip(xs, gs)):
        x_turned[:, at * count : (at + 1) * count] = x[...].T
        g_turned[:, at * count : (at + 1) * count] = g[...].T
    for block in range(blocks):
        some = pl.ds(pl.multiple_of((place_ref[CHIP] ^ block) * size, size), size)
        product = lambda turned, parts: sum(mm(turned[some, at * 2 * count : (at + 1) * 2 * count], part[...]) for at, part in enumerate(parts))
        to = up_send if block % 2 else up_keep
        to[block // 2] = product(x_turned, backs).astype(LOW)
        to = down_send if block >= blocks // 2 else down_keep
        to[block % (blocks // 2)] = product(g_turned, acts).astype(LOW)


def weigh(place, xs, gs, acts, backs, chips):
    count, width = xs[0].shape
    hidden = acts[0].shape[1]
    rows = len(xs) * count
    return pl.pallas_call(
        weigh_kernel,
        in_specs=[in_smem()] + [in_vmem()] * (2 * len(xs) + 2 * len(acts)),
        out_specs=[in_vmem()] * 4,
        out_shape=[shaped((chips // 2, width // chips, hidden), LOW)] * 4,
        scratch_shapes=[pltpu.VMEM((width, rows), LOW)] * 2,
        compiler_params=params(40),
        cost_estimate=pl.CostEstimate(flops=4 * rows * width * hidden, bytes_accessed=4 * width * hidden + 8 * rows * width, transcendentals=0),
        name="weigh",
    )(place, *xs, *gs, *acts, *backs)


def turn_kernel(*refs):
    out = refs[-1]
    for at, ref in enumerate(refs[:-1]):
        count = ref.shape[0]
        out[:, at * count : (at + 1) * count] = ref[...].T


def turn(parts):
    count, width = parts[0].shape
    return pl.pallas_call(
        turn_kernel,
        in_specs=[in_vmem()] * len(parts),
        out_specs=in_vmem(),
        out_shape=shaped((width, len(parts) * count), LOW),
        compiler_params=params(40),
        cost_estimate=pl.CostEstimate(flops=0, bytes_accessed=4 * len(parts) * count * width, transcendentals=0),
        name="turn",
    )(*parts)


def weigh_late_kernel(place_ref, turned_ref, projected_ref, weight_ref, context_ref, *refs):
    members = len(refs) - 7
    lows, (one_keep, one_send, two_keep, two_send, gain_ref, sums_ref, out_turned) = refs[:members], refs[members:]
    count = lows[0].shape[0]
    blocks, size, cols = 2 * one_keep.shape[0], one_keep.shape[1], one_keep.shape[2]
    out = sum(mm(context_ref[:, pl.ds(offset(place_ref, slot, count), count)], low[...]) for slot, low in enumerate(lows))
    out_turned[...] = out.T.astype(LOW)
    sums = jnp.sum(projected_ref[...].astype(WIDE), 0, keepdims=True)
    sums_ref[...] = sums
    for block in range(blocks):
        some = pl.ds(pl.multiple_of((place_ref[CHIP] ^ block) * size, size), size)
        product = mm(turned_ref[some, :], projected_ref[...])
        weight = weight_ref[some, : product.shape[1]].astype(WIDE)
        gain = jnp.sum(product * weight, 1, keepdims=True)
        shift = jnp.sum(sums * weight, 1, keepdims=True)
        lane = lax.broadcasted_iota(jnp.int32, (size, gain_ref.shape[1]), 1)
        gain_ref[some, :] = jnp.where(lane == 0, gain, shift)
        to = one_send if block % 2 else one_keep
        to[block // 2] = product[:, :cols].astype(LOW)
        to = two_send if block >= blocks // 2 else two_keep
        rest = product.shape[1] - cols
        to[block % (blocks // 2), :, :rest] = product[:, cols:].astype(LOW)
        to[block % (blocks // 2), :, rest:] = out_turned[some, :]


def weigh_late(place, turned, projected, weight, context, lows, chips):
    width, rows = turned.shape
    part = context.shape[0]
    cols = 2 * part
    return pl.pallas_call(
        weigh_late_kernel,
        in_specs=[in_smem()] + [in_vmem()] * (4 + len(lows)),
        out_specs=[in_vmem()] * 6,
        out_shape=[shaped((chips // 2, width // chips, cols), LOW)] * 4
        + [shaped((width, 128), WIDE), shaped((1, 3 * part), WIDE)],
        scratch_shapes=[pltpu.VMEM((width, part), LOW)],
        compiler_params=params(32),
        cost_estimate=pl.CostEstimate(flops=8 * rows * width * part, bytes_accessed=4 * rows * width + 12 * width * part, transcendentals=0),
        name="weigh_late",
    )(place, turned, projected, weight, context, *lows)


def share_kernel(projected_ref, weight_ref, zero_ref, one_ref, high_ref):
    count = zero_ref.shape[0]
    high_ref[...] = over_cols(projected_ref[2 * count :, :], weight_ref[...]).astype(LOW)
    one_ref[...] = over_cols(projected_ref[count : 2 * count, :], weight_ref[...]).astype(LOW)
    zero_ref[...] = over_cols(projected_ref[:count, :], weight_ref[...])


def share(projected, weight):
    rows, width = projected.shape[0], weight.shape[0]
    return pl.pallas_call(
        share_kernel,
        in_specs=[in_vmem()] * 2,
        out_specs=[in_vmem()] * 3,
        out_shape=[shaped((rows // 4, width), WIDE), shaped((rows // 4, width), LOW), shaped((rows // 2, width), LOW)],
        compiler_params=params(40),
        cost_estimate=pl.CostEstimate(flops=2 * rows * width * weight.shape[1], bytes_accessed=6 * rows * width, transcendentals=0),
        name="share",
    )(projected, weight)


def flip(size, bit):
    return [(at, at ^ bit) for at in range(size)]


def add_low(kept, taken):
    return (kept.astype(WIDE) + taken.astype(WIDE)).astype(LOW)


def add_up(values, axis, wide):
    size, bit = lax.axis_size(axis), 1
    while bit < size:
        mate = lax.ppermute(values, axis, flip(size, bit))
        if wide and 2 * bit < size:
            values = (values + mate) + (lax.ppermute(values, axis, flip(size, 2 * bit)) + lax.ppermute(values, axis, flip(size, 3 * bit)))
            bit *= 2
        else:
            values = values + mate
        bit *= 2
    return values

PLAN = {'first': (None, 1), 'notes': (None, 0), 'cotangent': (3, 6), 'second': (None, 3), 'pieces': (None, 2), 'outs': (None, 4), 'seconds': (None, 70), 'last': (None, 5), 'cotmate': (None, 7), 'cotnear': (None, 8), 'secnear': (None, 8), 'two': (11, 12), 'three': (11, None), 'fed': (None, 15), 'out': (None, 14), 'low': (None, 16), 'fedrest': (None, 16), 'hand': (None, None), 'output': (None, 16), 'late': (None, 20), 'laterest': (None, 21), 'latehand': (None, None), 'early': 1, 'half': 1, 'sums': 19, 'middle': 20, 'wide': 0, 'lateend': 1}


class Box:
    def __init__(self, value=None, at=None):
        self.value, self.at = value, at


class Order:
    def __init__(self):
        self.boxes, self.later = [], {}

    def keep(self, value, at):
        box = Box(value, at)
        self.boxes.append(box)
        return box

    def point(self, at, *values):
        boxes = [box for box in self.boxes if box.at == at]
        if boxes:
            tied = lax.optimization_barrier((*values, *[box.value for box in boxes]))
            values = tied[: len(values)]
            for box, value in zip(boxes, tied[len(values) :]):
                box.value, box.at = value, None
        for action in self.later.pop(at, ()):
            action()
        return values if len(values) > 1 else values[0]

    def send(self, name, operand, move):
        start, end = PLAN[name]
        result = Box()

        def go():
            with jax.named_scope(name):
                result.value = move(operand.value)
            result.at = end
            self.boxes.append(result)

        if start is None:
            go()
        else:
            operand.at = start
            if operand not in self.boxes:
                self.boxes.append(operand)
            self.later.setdefault(start, []).append(go)
        return result


def body(hidden, lengths, first_gain, first_shift, projection_in, query_value_bias, projection_out, out_bias,
         second_gain, second_shift, up_weight, up_bias, down_weight, down_bias, cotangent):
    rows, width = hidden.shape
    heads_width = projection_in.shape[2]
    hidden_width = up_weight.shape[1]
    groups, members = lax.axis_size("dp"), lax.axis_size("mp")
    group, member = lax.axis_index("dp"), lax.axis_index("mp")
    chips = groups // 2
    core, chip = group % 2, group // 2
    size, count = width // chips, width // groups
    scale = HEAD_DIM ** (-0.5)
    at_home = core == member // 2
    shard = jnp.where(at_home, member, member ^ 2)
    both = ("dp", "mp")
    away = [(at * 2 + 1 - z // 2, z) for at in range(chips) for z in range(members)]
    spot = lambda dp, mp: dp * members + mp
    far_pairs = [(spot(d, z), spot(d ^ 1, z ^ 2)) for d, z in away]
    near_mate_pairs = [(spot(d, z), spot(d ^ 1, z ^ 1)) for d in range(groups) for z in range(members)]
    hand_pairs = [(spot(d, z), spot(d, z ^ 2)) for d, z in away] + [(spot(d ^ 1, z), spot(d, z)) for d, z in away]
    away_pairs = lambda bit: [(spot(d, z), spot(d ^ (2 * bit), z)) for d, z in away]
    far = lambda value: lax.ppermute(value, both, far_pairs)
    mate = lambda value: lax.ppermute(value, "dp", flip(groups, 1))
    near = lambda value: lax.ppermute(value, "mp", flip(members, 1))
    near_mate = lambda value: lax.ppermute(value, both, near_mate_pairs)
    cross = lambda bit: lambda value: lax.ppermute(value, "dp", flip(groups, 2 * bit))
    row = lambda vector: vector.reshape(1, -1)
    order = Order()
    keep, point, send = order.keep, order.point, order.send
    pick = lambda own, got: jnp.where(at_home, own, got)

    def spread(name, piece):
        return [piece] + [send(name, keep(piece.value, None), lambda value, block=block: lax.ppermute(value, both, away_pairs(block))) for block in range(1, chips)]

    block_of = lambda value, axis: lax.dynamic_slice_in_dim(value, chip * size, size, axis)
    first_piece = jnp.concatenate([block_of(projection_in, 0).reshape(size, -1), block_of(projection_out, 1).T], 1)
    notes = jnp.concatenate([query_value_bias.reshape(-1), up_bias.astype(WIDE), jnp.broadcast_to(lengths.astype(WIDE), (512,))])
    first_far = send("first", keep(first_piece, None), far)
    notes_far = send("notes", keep(notes.reshape(-1, 128), None), far)
    cotangent_far = send("cotangent", keep(cotangent, None), far)
    second_piece = jnp.concatenate([block_of(up_weight, 0), block_of(down_weight, 0)], 0)
    second_far = send("second", keep(second_piece, None), far)
    hidden_own = pick(hidden, point(0, far(hidden)))
    notes = pick(notes, notes_far.value.reshape(-1))
    qv_bias = notes[: 2 * heads_width].reshape(2, heads_width)
    up_bias_own = row(notes[2 * heads_width : 2 * heads_width + hidden_width])
    length = notes[-1].astype(jnp.int32)
    place = jnp.stack([shard, chip, length, at_home.astype(jnp.int32)]).astype(jnp.int32)
    first_hat, first_inverse = normalize(hidden_own.astype(WIDE))
    first_own = (first_hat * first_gain + first_shift).astype(LOW)
    zero = jnp.zeros((heads_width,), WIDE)
    bias_flat = row(jnp.concatenate([qv_bias[0] * scale, zero, qv_bias[1]]))
    scale_flat = row(jnp.concatenate([zero + scale, zero + 1.0, zero + 1.0]))

    first_own = point(1, first_own)
    first_pieces = spread("pieces", first_far)
    first_near, first_mate = point(2, near(first_own), mate(first_own))
    firsts = [first_own, first_near, first_mate, mate(first_near)]
    *parts, weight_flat, out_own = open_up(
        place, projection_in.transpose(1, 0, 2), projection_out, scale_flat, bias_flat, [piece.value for piece in first_pieces], firsts
    )

    parts[1], out_own = point(3, parts[1], out_own)
    out_near, out_mate = send("outs", keep(out_own, None), near), send("outs", keep(out_own, None), mate)
    out_own = out_own
    turned, total, *context = attend(place, parts)
    context[1], context[2], context[3] = point(4, context[1], context[2], context[3])
    if second_far.value is not None:
        second_pieces = spread("seconds", second_far)
    out_last = send("last", keep(out_near.value, None), mate)
    exchange = (lambda value: value, near, mate, near_mate)
    context = [move(part) for move, part in zip(exchange, context)]
    context[1], context[2], context[3] = point(5, context[1], context[2], context[3])
    outs = [out_own, out_near.value, out_mate.value, out_last.value]
    middle, second_own = project(context, outs, hidden_own, row(out_bias), row(second_gain), row(second_shift))

    second_own = point(6, second_own)
    cotangent_own = keep(pick(cotangent, cotangent_far.value), None)
    second_mate, cotangent_mate, second_own, cotangent_own.value = point(
        7, mate(second_own), mate(cotangent_own.value), second_own, cotangent_own.value
    )
    second_near = send("secnear", keep(second_own, None), near)
    cotangent_near = send("cotnear", keep(cotangent_own.value, None), near)
    second_mate = point(70, second_mate)
    fed_weights = (up_bias_own, up_weight, down_weight, [piece.value for piece in second_pieces])
    act_one, back_one, bias_one, out_zero, grad_zero, other_two = feed(
        place, second_own, second_mate, cotangent_own.value, cotangent_mate, *fed_weights, True
    )
    act_one, other_two = point(8, act_one, other_two)
    two_got = send("two", keep(other_two, None), mate)
    second_near.value, cotangent_near.value = point(9, second_near.value, cotangent_near.value)
    second_last, cotangent_last = mate(second_near.value), mate(cotangent_near.value)
    act_two, back_two, bias_two, out_one, grad_one, other_three = feed(
        place, second_near.value, second_last, cotangent_near.value, cotangent_last, *fed_weights, False
    )
    three_got = mate(point(10, other_three))
    grad_next = add_low(grad_one, three_got[rows:])
    grad_near = near(grad_next)
    second_keep, grad_next = point(11, second_own, grad_next)
    up_keep, up_send, down_keep, down_send = weigh(
        place,
        [second_keep, second_mate, second_near.value, second_last],
        [cotangent_own.value, cotangent_mate, cotangent_near.value, cotangent_last],
        [act_one, act_two],
        [back_one, back_two],
        chips,
    )
    up_got = send("fed", keep(up_send, None), cross(1))
    down_got = send("fed", keep(down_send, None), cross(chips // 2))
    grad_near, up_keep = point(12, grad_near, up_keep)
    low_middle, back_middle, sums_part, *back_context = unproject(
        grad_zero, two_got.value, grad_near, middle, cotangent_own.value, row(second_gain), outs
    )
    out_next = add_low(out_one, three_got[:rows])
    out_sum = send("out", keep(out_next, None), near)

    back_context[1], low_middle = point(13, back_context[1], low_middle)
    back_context = [move(part) for move, part in zip(exchange, back_context)]
    first_turned = keep(turn(firsts), 14)
    back_context[1], back_context[2], back_context[3], low_middle = point(14, back_context[1], back_context[2], back_context[3], low_middle)

    def halved(up_keep, up_got, down_keep, down_got):
        return add_low(up_keep, up_got), add_low(down_keep, down_got)

    def handed(name, value):
        rows_of = lambda at: lax.dynamic_slice_in_dim(value, at * count, count, 0)
        kept, given = rows_of(member // 2), rows_of(1 - member // 2)
        return kept, send(name, keep(kept, None), far), send(name, keep(given, None), lambda value: lax.ppermute(value, both, hand_pairs))

    settled = lambda kept, got_far, got: pick(kept, got_far.value).astype(WIDE) + got.value.astype(WIDE)
    low_mate, low_near = send("low", keep(low_middle, None), mate), send("low", keep(low_middle, None), near)
    written = lambda: (middle + out_zero + two_got.value[:rows].astype(WIDE) + out_sum.value.astype(WIDE) + down_bias).astype(LOW)
    if PLAN["early"]:
        output = keep(written(), 15)
    back_context[1], up_keep, down_keep = point(15, back_context[1], up_keep, down_keep)
    up_sum, down_sum = halved(up_keep, up_got.value, down_keep, down_got.value) if PLAN["half"] else (None, None)

    def rest(up_sum, down_sum, name):
        bit, sent = 2, []
        while bit < chips:
            half = down_sum.shape[0] // 2
            sent = send(name, keep(up_sum[1::2], None), cross(bit)), send(name, keep(down_sum[half:], None), cross(chips // 2 // bit))
            bit *= 2
            if bit < chips:
                up_sum, down_sum = halved(up_sum[0::2], sent[0].value, down_sum[:half], sent[1].value)
        return up_sum[0::2], sent[0], down_sum[: down_sum.shape[0] // 2], sent[1]

    def finish(up_keep, up_got, down_keep, down_got):
        up_sum, down_sum = halved(up_keep, up_got.value, down_keep, down_got.value)
        return jnp.concatenate([up_sum[0], down_sum[0]], 1)

    if PLAN["half"]:
        fed_rest = rest(up_sum, down_sum, "fedrest")
    if PLAN["early"]:
        output_far = send("output", keep(output.value, None), far)
    back_projected = attend_back(place, parts, back_context, turned, total)
    back_projected = point(16, back_projected)
    lows = [low_middle, low_near.value, low_mate.value, mate(low_near.value)]

    if not PLAN["half"]:
        up_sum, down_sum = halved(up_keep, up_got.value, down_keep, down_got.value)
        up_sum, back_projected = lax.optimization_barrier((up_sum, back_projected))
        fed_rest = rest(up_sum, down_sum, "fedrest")
    if PLAN["half"]:
        fed_sum = finish(*fed_rest)
        fed_sum, back_projected = lax.optimization_barrier((fed_sum, back_projected))
        fed_parts = handed("hand", fed_sum)
    share_zero, share_one, share_high = share(back_projected, weight_flat)
    share_high, back_projected = point(17, share_high, back_projected)
    share_got = mate(share_high)
    share_zero, share_next, back_projected = point(
        18, share_zero + share_got[:rows].astype(WIDE), add_low(share_one, share_got[rows:]), back_projected
    )
    share_near = near(share_next)
    *late_parts, late_gains, projected_sums = weigh_late(place, first_turned.value, back_projected, weight_flat, turned, lows, chips)
    late_parts[1], late_parts[3], share_zero = point(19, late_parts[1], late_parts[3], share_zero)
    late_up, late_down = send("late", keep(late_parts[1], None), cross(1)), send("late", keep(late_parts[3], None), cross(chips // 2))
    gains = keep(late_gains, PLAN["sums"])
    if not PLAN["early"]:
        output_far = send("output", keep(written(), None), far)
    if not PLAN["half"]:
        fed_parts = handed("hand", finish(*fed_rest))

    def gather_sums():
        placed = lambda value, whole: lax.dynamic_update_slice(jnp.zeros((whole,), WIDE), value, (shard * value.shape[0],))
        shift_grad = gains.value[:, 1]
        sums = [
            (gains.value[:, 0] - first_shift * shift_grad) / first_gain,
            shift_grad,
            placed(projected_sums[0, :heads_width], width),
            placed(projected_sums[0, 2 * heads_width :], width),
            sums_part[:4].reshape(-1),
            placed((bias_one + bias_two)[0], members * hidden_width),
        ]
        return add_up(jnp.concatenate(sums).reshape(-1, 128), "dp", PLAN["wide"])

    if PLAN["sums"] != 20:
        sums = keep(gather_sums(), PLAN["middle"])
    share_near, share_zero = point(20, share_near, share_zero)
    if PLAN["sums"] == 20:
        sums = keep(gather_sums(), PLAN["middle"])
    late_rest = rest(*halved(late_parts[0], late_up.value, late_parts[2], late_down.value), "laterest")
    if PLAN["lateend"] == 0:
        late_end = handed("latehand", finish(*late_rest))
    back_first = share_zero + share_near.astype(WIDE)
    hidden_grad = (back_middle + norm_back(back_first, first_hat, first_inverse, first_gain)).astype(LOW)
    hidden_grad = point(21, hidden_grad)
    hidden_grad_far = far(hidden_grad)
    if PLAN["lateend"] == 1:
        late_end = handed("latehand", finish(*late_rest))
    sums = add_up(sums.value, "mp", PLAN["wide"]).reshape(-1)
    fed_grad, late_grad = settled(*fed_parts), settled(*late_end)
    small = [sums[at * width : (at + 1) * width] for at in range(8)]
    return (
        pick(output.value if PLAN["early"] else written(), output_far.value),
        pick(hidden_grad, hidden_grad_far),
        small[0],
        small[1],
        late_grad[:, : 3 * heads_width].reshape(-1, 3, heads_width),
        sums[2 * width : 4 * width].reshape(2, width),
        late_grad[:, 3 * heads_width :].T,
        small[6],
        small[4],
        small[5],
        fed_grad[:, :hidden_width],
        sums[8 * width :],
        fed_grad[:, hidden_width:].T,
        small[7],
    )


def solution(mesh):
    placed = (
        P(("dp", "mp"), None),
        P("dp"),
        P(),
        P(),
        P(None, None, "mp"),
        P(None, "mp"),
        P("mp", None),
        P(),
        P(),
        P(),
        P(None, "mp"),
        P("mp"),
        P("mp", None),
        P(),
        P(("dp", "mp"), None),
    )
    return jax.shard_map(
        body,
        mesh=mesh,
        in_specs=placed,
        out_specs=(
            P(("dp", "mp"), None),
            P(("dp", "mp"), None),
            P(),
            P(),
            P("dp", None, "mp"),
            P(),
            P("mp", "dp"),
            P(),
            P(),
            P(),
            P("dp", "mp"),
            P(),
            P("mp", "dp"),
            P(),
        ),
        check_vma=False,
    )
```
